32 devices in a mesh: tm: 4 (over y, x), space: 8 (over z, core).
Axes of the slice: x: 2, y: 2, z: 4, core: 2. Of those that a mesh axis runs over, the one named last changes fastest.
Arguments:
- fields: bfloat16 [4096, 2, 16384], P('tm', None, 'space')
- calendar_day: int32 [4096], P('tm'), may hold values from 0 to 364, as said below
- events: int32 [16, 96], replicated, may hold values from 0 to 4080, as said below
- lag_offsets: int32 [16], replicated, may hold values from 0 to 15, each once
Outputs:
- composite: float32 [16, 16, 2, 16384], P('tm', None, None, 'space')
The draws below stay inside these ranges and needn't reach their ends.
Inputs may be any that keep to these rules, and one draw needn't show every extreme that they name: `calendar_day`: days of the year of successive record days, one or two calendar days apart. `events`: each entry is a record day; a day may repeat within a type. `lag_offsets`: each of 0 to 15 once.
All inputs are finite; a program needn't handle non-finite values.
Results may differ from the reference program's by a relative error of at most 0.0012.
Values may be sent and summed in bfloat16 or wider, within the bound.
A program may use at most 64 MiB of HBM per device.

```python
import jax
import jax.numpy as jnp
from jax import lax

TYPES = 16
LAGS = 16
MEMBERS = 96
HARMONICS = 4
DAYS = 4096
POINTS = 16384


TWO_PI = 6.283185307179586


def calendar_draw(key):
    day_steps = jax.random.randint(jax.random.fold_in(key, 11), (DAYS,), 1, 3)
    first_day = jax.random.randint(jax.random.fold_in(key, 12), (), 0, 365)
    return jnp.mod(first_day + jnp.cumsum(day_steps), 365).astype(jnp.int32)


def draw_calendar_day(key, part):
    return calendar_draw(key)


def draw_events(key, part):
    early_pick = jax.random.randint(jax.random.fold_in(key, 21), (TYPES, MEMBERS), 0, DAYS - LAGS + 1)
    later_pick = jax.random.randint(jax.random.fold_in(key, 22), (TYPES, MEMBERS), 0, DAYS - LAGS + 1)
    chosen = jnp.minimum(early_pick, later_pick)
    chosen = chosen.at[0, 0].set(DAYS - LAGS).at[1, 0].set(0)
    return chosen.astype(jnp.int32)


def draw_fields(key, part):
    calendar_days = calendar_draw(key)
    phases = calendar_days.astype(jnp.float32) * (TWO_PI / 365.25)
    orders = jnp.arange(1, HARMONICS + 1).astype(jnp.float32)
    angles = phases[:, None] * orders[None, :]
    basis = jnp.concatenate([jnp.cos(angles), jnp.sin(angles)], axis=1)
    subkeys = jax.random.split(jax.random.fold_in(key, 31), 6)
    scaling = jnp.concatenate([orders, orders])
    amplitudes = jax.random.normal(subkeys[0], (2 * HARMONICS, 2 * POINTS), jnp.float32) * 1.5 / scaling[:, None]
    seasonal = jnp.dot(basis, amplitudes, precision=lax.Precision.HIGHEST)
    position = (jnp.arange(2 * POINTS) % POINTS).astype(jnp.float32) / POINTS
    ramp_factor = 1.0 + 2.0 * position
    levels = jax.random.uniform(subkeys[1], (2 * POINTS,), jnp.float32, 0.5, 1.5) * ramp_factor
    offset = jax.random.normal(subkeys[2], (2 * POINTS,), jnp.float32) * 3.0
    fraction = jnp.arange(DAYS).astype(jnp.float32) / DAYS
    noise_part = jax.random.normal(subkeys[3], (DAYS, 2 * POINTS), jnp.float32) * 0.8
    combined = seasonal + offset[None, :] + 2.0 * fraction[:, None] * levels[None, :] + noise_part * ramp_factor[None, :]
    return combined.reshape(DAYS, 2, POINTS).astype(jnp.bfloat16)


def setup_inputs(seed: int = 0) -> dict:
    streams_of = jax.random.split(jax.random.key(seed), 5)
    return {
        "fields": draw_fields(jax.random.fold_in(streams_of[4], 71), 0),
        "calendar_day": draw_calendar_day(jax.random.fold_in(streams_of[4], 71), 0),
        "events": draw_events(jax.random.fold_in(streams_of[4], 71), 0),
        "lag_offsets": jax.random.permutation(streams_of[3], LAGS).astype(jnp.int32),
    }


TWO_PI = 6.283185307179586

def regressors(calendar_day):
    phases = calendar_day.astype(jnp.float32) * (TWO_PI / 365.25)
    columns = [jnp.ones_like(phases)]
    for harmonic in range(1, HARMONICS + 1):
        columns.append(jnp.cos(harmonic * phases))
        columns.append(jnp.sin(harmonic * phases))
    return jnp.stack(columns, axis=1).astype(jnp.bfloat16)

def solve_fit(gram_matrix, projection):
    factor = jnp.linalg.cholesky(gram_matrix)
    return jax.scipy.linalg.cho_solve((factor, True), projection)

def reference(fields, calendar_day, events, lag_offsets):
    design = regressors(calendar_day)
    record = fields.reshape(DAYS, 2 * POINTS)
    gram_matrix = jnp.dot(design.T.astype(jnp.float32), design.astype(jnp.float32), preferred_element_type=jnp.float32)
    projection = jnp.dot(design.T.astype(jnp.float32), record.astype(jnp.float32), preferred_element_type=jnp.float32)
    coefficients = solve_fit(gram_matrix, projection)
    design_wide = design.astype(jnp.float32)

    def type_sums(event_row):
        chosen = (event_row[:, None] + lag_offsets[None, :]).astype(jnp.int32).reshape(-1)
        picked = jnp.take(record, chosen, axis=0).reshape(MEMBERS, LAGS, 2 * POINTS)
        raw_sums = jnp.sum(picked.astype(jnp.float32), axis=0)
        picked_design = jnp.take(design_wide, chosen, axis=0).reshape(MEMBERS, LAGS, 2 * HARMONICS + 1)
        counted_design = jnp.sum(picked_design, axis=0)
        return raw_sums - jnp.dot(counted_design, coefficients, precision=lax.Precision.HIGHEST)
    totals = lax.map(type_sums, events)
    maps = (totals / MEMBERS).reshape(TYPES, LAGS, 2, POINTS)
    map_mean = jnp.sum(maps, axis=3, keepdims=True) / POINTS
    return maps - map_mean
```

```python
import functools

import jax
import jax.numpy as jnp
from jax import lax
from jax.experimental import pallas as pl
from jax.experimental.pallas import tpu as pltpu
from jax.sharding import PartitionSpec as P

HARMONICS = 4
TERMS = 2 * HARMONICS + 1
TWO_PI = 6.283185307179586
LANES = 128
PAD = 128
CHUNK = 256
AHEAD = 4
NN = (((1,), (0,)), ((), ()))
NT = (((1,), (1,)), ((), ()))
TN = (((0,), (0,)), ((), ()))


def split3(value):
    high = value.astype(jnp.bfloat16)
    rest = value - high.astype(jnp.float32)
    middle = rest.astype(jnp.bfloat16)
    low = (rest - middle.astype(jnp.float32)).astype(jnp.bfloat16)
    return high, middle, low


def encode(part):
    top = jnp.max(jnp.abs(part), axis=0, keepdims=True)
    factor = jnp.where(top > 0.0, 32767.0 / jnp.where(top > 0.0, top, 1.0), 0.0)
    return jnp.round(part * factor).astype(jnp.int32).astype(jnp.int16), top * (1.0 / 32767.0)


def decode(codes, scale):
    return codes.astype(jnp.int32).astype(jnp.float32) * scale


def flip(index, bits):
    bit = 1
    flipped = index
    while bit <= bits:
        if bits & bit:
            flipped = flipped + bit - 2 * bit * lax.rem(lax.div(index, bit), 2)
        bit *= 2
    return flipped


def ones_where(condition):
    return jnp.where(condition, 1.0, 0.0).astype(jnp.bfloat16)


def count_weights(places, weights_ref, depth):
    types, members = places.shape
    shifts = (weights_ref.shape[0] - 32) // types
    tiles = (depth + PAD) // LANES
    upper = lax.shift_right_arithmetic(places, 7)
    lower = lax.bitwise_and(places, LANES - 1)
    tile_lines = lax.broadcasted_iota(jnp.int32, (-(-tiles // 8) * 8, members), 0)
    lane_lines = lax.broadcasted_iota(jnp.int32, (LANES, members), 0)
    for kind in range(types):
        in_tile = ones_where(upper[kind : kind + 1, :] == tile_lines)
        in_lane = ones_where(lower[kind : kind + 1, :] == lane_lines)
        histogram = lax.dot_general(in_tile, in_lane, NT, preferred_element_type=jnp.float32)
        wide = jnp.concatenate(
            [jnp.broadcast_to(histogram[tile : tile + 1, :], (shifts, LANES)) for tile in range(tiles)], axis=1
        )
        rolled = pltpu.roll(wide, 0, 1, stride=1, stride_axis=0)
        weights_ref[kind * shifts : (kind + 1) * shifts, :] = rolled[:, PAD:].astype(jnp.bfloat16)


def regressors(calendar, weights_ref):
    phase = calendar.astype(jnp.float32) * (TWO_PI / 365.25)
    cosines, sines = [jnp.cos(phase)], [jnp.sin(phase)]
    for order in range(2, HARMONICS + 1):
        a, b = order // 2 - 1, order - order // 2 - 1
        cosines.append(cosines[a] * cosines[b] - sines[a] * sines[b])
        sines.append(sines[a] * cosines[b] + cosines[a] * sines[b])
    terms = [jnp.ones_like(phase)]
    for order in range(HARMONICS):
        terms += [cosines[order], sines[order]]
    tiles = calendar.shape[0]
    line = lax.broadcasted_iota(jnp.int32, (16, LANES), 0)
    blocks = []
    for tile in range(tiles):
        block = jnp.zeros((16, LANES), jnp.float32)
        for term, values in enumerate(terms):
            block = jnp.where(line == term, values[tile : tile + 1, :], block)
        blocks.append(block)
    stacked = jnp.concatenate(blocks, axis=0).astype(jnp.bfloat16)
    day = lax.broadcasted_iota(jnp.int32, (LANES, 2 * LANES), 0)
    place = lax.broadcasted_iota(jnp.int32, (LANES, 2 * LANES), 1)
    first = ones_where(place == 2 * day)
    second = ones_where(place == 2 * day + 1)
    base = weights_ref.shape[0] - 32
    spread = []
    for matrix in (first, second):
        wide = jnp.dot(stacked, matrix, preferred_element_type=jnp.float32)
        spread.append(jnp.concatenate([wide[16 * tile : 16 * tile + 16, :] for tile in range(tiles)], axis=1))
    weights_ref[base : base + 16, :] = spread[0].astype(jnp.bfloat16)
    weights_ref[base + 16 :, :] = spread[1].astype(jnp.bfloat16)
    return (spread[0] + spread[1]).astype(jnp.bfloat16)


def solve(system, count_rows):
    lines = lax.broadcasted_iota(jnp.int32, (16, LANES), 0)
    columns = [
        jnp.broadcast_to(system[:, count_rows + k : count_rows + k + 1], (16, LANES)) for k in range(TERMS)
    ]
    sides = [system[:, start : start + LANES] for start in range(0, count_rows, LANES)]
    for k in range(TERMS):
        column = columns[k]
        inverse = 1.0 / column[k : k + 1, :]

        def eliminate(block):
            pivot = block[k : k + 1, :] * inverse
            return jnp.where(lines == k, pivot, block - column * pivot)

        sides = [eliminate(block) for block in sides]
        columns = [eliminate(block) if j > k else block for j, block in enumerate(columns)]
    return jnp.concatenate([jnp.where(lines < TERMS, block, 0.0) for block in sides], axis=1)


def compose(
    tm, space, members, all_points,
    fields, calendar, events, out_ref,
    xs, calendar_ref, events_ref, weights_ref, normal_ref, normals, left, raws, whole, spatial, parts,
    sums, got_sums, totals, got_totals, means, codes, scales, got_codes, got_scales,
    x_sems, in_sems, n_send, n_recv, m_send, m_recv, t_send, t_recv, c_send, c_recv, s_send, s_recv,
):
    chunks, days = xs.shape[0], xs.shape[1]
    depth = weights_ref.shape[1]
    count_rows = weights_ref.shape[0] - 32
    rows = count_rows // tm
    me = lax.axis_index("tm")
    here = lax.axis_index("space")
    stages = tm.bit_length() - 1

    def load(c):
        return pltpu.make_async_copy(
            fields.at[:, :, pl.ds(pl.multiple_of(c * CHUNK, CHUNK), CHUNK)], xs.at[c], x_sems.at[c]
        )

    barrier = pltpu.get_barrier_semaphore()
    for i in range(1, tm):
        pl.semaphore_signal(barrier, inc=1, device_id={"tm": lax.rem(me + i, tm)})
    for i in range(1, space):
        pl.semaphore_signal(barrier, inc=1, device_id={"space": lax.rem(here + i, space)})
    load_events = pltpu.make_async_copy(events, events_ref, in_sems.at[0])
    load_calendar = pltpu.make_async_copy(calendar, calendar_ref, in_sems.at[1])
    load_events.start()
    load_calendar.start()
    lax.fori_loop(0, chunks, lambda c, _: (load(c).start(), 0)[1], 0)

    def send_normal(i):
        return pltpu.make_async_remote_copy(
            normal_ref, normals.at[i - 1], n_send.at[i - 1], n_recv.at[i - 1], device_id={"tm": lax.rem(me + i, tm)}
        )

    def send_sums(i):
        return pltpu.make_async_remote_copy(
            sums, got_sums.at[i - 1], m_send.at[i - 1], m_recv.at[i - 1],
            device_id={"space": lax.rem(here + i, space)},
        )

    def send_totals(i):
        return pltpu.make_async_remote_copy(
            totals, got_totals.at[i - 1], t_send.at[i - 1], t_recv.at[i - 1],
            device_id={"tm": lax.rem(me + i, tm)},
        )

    def bits_of(turn):
        return [1 << ((turn + stage) % stages) for stage in range(stages)]

    def leaving(turn, stage):
        bits = bits_of(turn)
        return [
            apart for apart in range(1, tm)
            if apart & bits[stage] and not any(apart & bit for bit in bits[:stage])
        ]

    def first_slot(stage):
        return tm - (tm >> stage)

    def send_codes(c, turn, stage):
        peer = {"tm": flip(me, bits_of(turn)[stage])}
        slots = pl.ds(first_slot(stage), tm >> (stage + 1))
        return (
            pltpu.make_async_remote_copy(
                codes.at[c, slots], got_codes.at[c, slots], c_send.at[stage, c], c_recv.at[stage, c], device_id=peer
            ),
            pltpu.make_async_remote_copy(
                scales.at[c, slots], got_scales.at[c, slots], s_send.at[stage, c], s_recv.at[stage, c], device_id=peer
            ),
        )

    load_events.wait()
    count_weights(2 * (events_ref[...] - me * days) + PAD, weights_ref, depth)
    load_calendar.wait()
    design = regressors(calendar_ref[...], weights_ref)
    normal_ref[...] = lax.dot_general(design, weights_ref[...], NT, preferred_element_type=jnp.float32)

    pl.semaphore_wait(barrier, tm + space - 2)
    for i in range(1, tm):
        send_normal(i).start()

    def multiply(c, carry):
        load(c).wait()
        raws[c] = jnp.dot(weights_ref[...], xs[c].reshape(depth, CHUNK), preferred_element_type=jnp.float32)
        return carry

    ahead = -(-AHEAD // stages) * stages
    lax.fori_loop(0, ahead, multiply, 0)

    system = normal_ref[...]
    for i in range(1, tm):
        send_normal(i).wait()
        system = system + normals[i - 1]
    fit = solve(system, count_rows)
    odd = lax.broadcasted_iota(jnp.int32, fit.shape, 1) % 2
    fit = jnp.concatenate([jnp.where(odd == 0, fit, 0.0), jnp.where(odd == 1, fit, 0.0)], axis=0)
    high, middle, low = [piece.astype(jnp.float32) for piece in split3(fit)]
    left[...] = jnp.transpose(jnp.concatenate([high, high, high, middle, middle, low], axis=0)).astype(jnp.bfloat16)
    spatial[...] = jnp.zeros_like(spatial)

    def grouped(body, start, stop):
        def group(g, carry):
            for turn in range(stages):
                body(start + g * stages + turn, turn)
            return carry

        assert (stop - start) % stages == 0
        lax.fori_loop(0, (stop - start) // stages, group, 0)

    def post(c, turn, stage):
        for slot, apart in enumerate(leaving(turn, stage)):
            place = first_slot(stage) + slot
            codes[c, place], scales[c, place] = encode(parts[apart, c])
        for copy in send_codes(c, turn, stage):
            copy.start()

    def collect(c, turn, stage):
        bit = bits_of(turn)[stage]
        for copy in send_codes(c, turn, stage):
            copy.wait_recv()
        for slot, apart in enumerate(leaving(turn, stage)):
            place = first_slot(stage) + slot
            parts[apart - bit, c] += decode(got_codes[c, place], got_scales[c, place])

    def anomalies(c, turn):
        p_high, p_middle, p_low = split3(raws[c, count_rows:, :])
        right = jnp.concatenate([p_high, p_middle, p_low, p_high, p_middle, p_high], axis=0)
        whole[...] = raws[c, :count_rows, :] - jnp.dot(left[...], right, preferred_element_type=jnp.float32)
        for apart in range(tm):
            parts[apart, c] = whole[pl.ds(pl.multiple_of(flip(me, apart) * rows, rows), rows), :]
        post(c, turn, 0)
        spatial[...] += whole[...]

    def both(c, turn):
        anomalies(c, turn)
        multiply(c + ahead, 0)

    grouped(both, 0, chunks - ahead)
    grouped(anomalies, chunks - ahead, chunks)

    ones = jnp.ones((8, CHUNK), jnp.bfloat16)
    total = jnp.zeros((8, count_rows), jnp.float32)
    for piece in split3(spatial[...]):
        total = total + lax.dot_general(ones, piece, NT, preferred_element_type=jnp.float32)
    sums[...] = total[0:1, :]
    for i in range(1, space):
        send_sums(i).start()

    half = chunks // 2

    def relay(stage):
        def body(c, turn):
            collect(c, turn, stage - 1)
            post(c, turn, stage)

        return body

    def spread_sums():
        total = sums[...]
        for i in range(1, space):
            send_sums(i).wait()
            total = total + got_sums[i - 1]
        totals[...] = total
        for i in range(1, tm):
            send_totals(i).start()

    for stage in range(1, stages):
        grouped(relay(stage), 0, half)
        if stage == 1:
            spread_sums()
        grouped(relay(stage), half, chunks)

    total = totals[...]
    for i in range(1, tm):
        send_totals(i).wait()
        total = total + got_totals[i - 1]
    means[...] = lax.dot_general(
        jnp.broadcast_to(total * (1.0 / (8 * members * all_points)), (8, count_rows)), jnp.ones((8, CHUNK), jnp.float32),
        TN, precision=lax.Precision.HIGHEST, preferred_element_type=jnp.float32,
    )

    def gather(c, turn):
        collect(c, turn, stages - 1)
        mean = means[pl.ds(pl.multiple_of(me * rows, rows), rows), :]
        value = parts[0, c] * (1.0 / members) - mean
        out_ref[:, :, :, pl.ds(pl.multiple_of(c * CHUNK, CHUNK), CHUNK)] = value.reshape(out_ref.shape[:3] + (CHUNK,))

    grouped(gather, 0, chunks)

    def sent(c, turn):
        for stage in range(stages):
            for copy in send_codes(c, turn, stage):
                copy.wait_send()

    grouped(sent, 0, chunks)


def finish(lags_ref, natural, out, sems):
    def copy(lag):
        return pltpu.make_async_copy(natural.at[:, lags_ref[lag]], out.at[:, lag], sems.at[lag])

    for lag in range(out.shape[1]):
        copy(lag).start()
    for lag in range(out.shape[1]):
        copy(lag).wait()


def shards(tm, space, fields, calendar_day, events, lag_offsets):
    types, members = events.shape
    lag_count = lag_offsets.shape[0]
    days, variables, points = fields.shape
    depth = variables * days
    count_rows = types * lag_count * variables
    rows = count_rows // tm
    chunks = points // CHUNK
    stages = tm.bit_length() - 1
    dma = pltpu.SemaphoreType.DMA
    vmem = pltpu.VMEM
    f32, bf16 = jnp.float32, jnp.bfloat16
    shape = (types // tm, lag_count, variables, points)
    natural = pl.pallas_call(
        functools.partial(compose, tm, space, members, points * space),
        out_shape=jax.ShapeDtypeStruct(shape, f32),
        in_specs=[pl.BlockSpec(memory_space=pltpu.HBM)] * 3,
        out_specs=pl.BlockSpec(memory_space=vmem),
        scratch_shapes=[
            vmem((chunks, days, variables, CHUNK), bf16),
            vmem((days // LANES, LANES), jnp.int32),
            vmem((types, members), jnp.int32),
            vmem((count_rows + 32, depth), bf16),
            vmem((16, count_rows + 32), f32),
            vmem((tm - 1, 16, count_rows + 32), f32),
            vmem((count_rows, 192), bf16),
            vmem((chunks, count_rows + 32, CHUNK), f32),
            vmem((count_rows, CHUNK), f32),
            vmem((count_rows, CHUNK), f32),
            vmem((tm, chunks, rows, CHUNK), f32),
            vmem((1, count_rows), f32),
            vmem((space - 1, 1, count_rows), f32),
            vmem((1, count_rows), f32),
            vmem((tm - 1, 1, count_rows), f32),
            vmem((count_rows, CHUNK), f32),
            vmem((chunks, tm - 1, rows, CHUNK), jnp.int16),
            vmem((chunks, tm - 1, 1, CHUNK), f32),
            vmem((chunks, tm - 1, rows, CHUNK), jnp.int16),
            vmem((chunks, tm - 1, 1, CHUNK), f32),
            dma((chunks,)), dma((2,)),
            dma((tm - 1,)), dma((tm - 1,)),
            dma((space - 1,)), dma((space - 1,)),
            dma((tm - 1,)), dma((tm - 1,)),
            dma((stages, chunks)), dma((stages, chunks)), dma((stages, chunks)), dma((stages, chunks)),
        ],
        compiler_params=pltpu.CompilerParams(
            collective_id=0, has_side_effects=True, vmem_limit_bytes=52 * 2**20
        ),
        name="compose",
    )(fields, calendar_day.reshape(days // LANES, LANES), events)
    return pl.pallas_call(
        finish,
        out_shape=jax.ShapeDtypeStruct(shape, f32),
        in_specs=[pl.BlockSpec(memory_space=pltpu.SMEM), pl.BlockSpec(memory_space=vmem)],
        out_specs=pl.BlockSpec(memory_space=pl.ANY),
        scratch_shapes=[dma((lag_count,))],
        compiler_params=pltpu.CompilerParams(vmem_limit_bytes=8 * 2**20),
        name="finish",
    )(lag_offsets, natural)


def solution(mesh):
    return jax.shard_map(
        functools.partial(shards, mesh.shape["tm"], mesh.shape["space"]),
        mesh=mesh,
        in_specs=(P("tm", None, "space"), P("tm"), P(), P()),
        out_specs=P("tm", None, None, "space"),
        check_vma=False,
    )
```

```python
import functools

import jax
import jax.numpy as jnp
from jax import lax
from jax.experimental import pallas as pl
from jax.experimental.pallas import tpu as pltpu
from jax.sharding import PartitionSpec as P

HARMONICS = 4
TERMS = 2 * HARMONICS + 1
TWO_PI = 6.283185307179586
LANES = 128
PAD = 128
CHUNK = 256
AHEAD = 4
NN = (((1,), (0,)), ((), ()))
NT = (((1,), (1,)), ((), ()))
TN = (((0,), (0,)), ((), ()))


def split3(value):
    high = value.astype(jnp.bfloat16)
    rest = value - high.astype(jnp.float32)
    middle = rest.astype(jnp.bfloat16)
    low = (rest - middle.astype(jnp.float32)).astype(jnp.bfloat16)
    return high, middle, low


def encode(part):
    top = jnp.max(jnp.abs(part), axis=0, keepdims=True)
    factor = jnp.where(top > 0.0, 32767.0 / jnp.where(top > 0.0, top, 1.0), 0.0)
    return jnp.round(part * factor).astype(jnp.int32).astype(jnp.int16), top * (1.0 / 32767.0)


def decode(codes, scale):
    return codes.astype(jnp.int32).astype(jnp.float32) * scale


def flip(index, bits):
    bit = 1
    flipped = index
    while bit <= bits:
        if bits & bit:
            flipped = flipped + bit - 2 * bit * lax.rem(lax.div(index, bit), 2)
        bit *= 2
    return flipped


def ones_where(condition):
    return jnp.where(condition, 1.0, 0.0).astype(jnp.bfloat16)


def count_weights(places, weights_ref, depth):
    types, members = places.shape
    lag_count = (weights_ref.shape[0] - 32) // (2 * types)
    tiles = (depth + PAD) // LANES
    upper = lax.shift_right_arithmetic(places, 7)
    lower = lax.bitwise_and(places, LANES - 1)
    tile_lines = lax.broadcasted_iota(jnp.int32, (-(-tiles // 8) * 8, members), 0)
    lane_lines = lax.broadcasted_iota(jnp.int32, (LANES, members), 0)
    for kind in range(types):
        in_tile = ones_where(upper[kind : kind + 1, :] == tile_lines)
        in_lane = ones_where(lower[kind : kind + 1, :] == lane_lines)
        histogram = lax.dot_general(in_tile, in_lane, NT, preferred_element_type=jnp.float32)
        wide = jnp.concatenate(
            [jnp.broadcast_to(histogram[tile : tile + 1, :], (lag_count, LANES)) for tile in range(tiles)], axis=1
        )
        for variable in range(2):
            rolled = pltpu.roll(wide, variable, 1, stride=2, stride_axis=0)
            start = (2 * kind + variable) * lag_count
            weights_ref[start : start + lag_count, :] = rolled[:, PAD:].astype(jnp.bfloat16)


def regressors(calendar, weights_ref):
    phase = calendar.astype(jnp.float32) * (TWO_PI / 365.25)
    cosines, sines = [jnp.cos(phase)], [jnp.sin(phase)]
    for order in range(2, HARMONICS + 1):
        a, b = order // 2 - 1, order - order // 2 - 1
        cosines.append(cosines[a] * cosines[b] - sines[a] * sines[b])
        sines.append(sines[a] * cosines[b] + cosines[a] * sines[b])
    terms = [jnp.ones_like(phase)]
    for order in range(HARMONICS):
        terms += [cosines[order], sines[order]]
    tiles = calendar.shape[0]
    line = lax.broadcasted_iota(jnp.int32, (16, LANES), 0)
    blocks = []
    for tile in range(tiles):
        block = jnp.zeros((16, LANES), jnp.float32)
        for term, values in enumerate(terms):
            block = jnp.where(line == term, values[tile : tile + 1, :], block)
        blocks.append(block)
    stacked = jnp.concatenate(blocks, axis=0).astype(jnp.bfloat16)
    day = lax.broadcasted_iota(jnp.int32, (LANES, 2 * LANES), 0)
    place = lax.broadcasted_iota(jnp.int32, (LANES, 2 * LANES), 1)
    first = ones_where(place == 2 * day)
    second = ones_where(place == 2 * day + 1)
    base = weights_ref.shape[0] - 32
    spread = []
    for matrix in (first, second):
        wide = jnp.dot(stacked, matrix, preferred_element_type=jnp.float32)
        spread.append(jnp.concatenate([wide[16 * tile : 16 * tile + 16, :] for tile in range(tiles)], axis=1))
    weights_ref[base : base + 16, :] = spread[0].astype(jnp.bfloat16)
    weights_ref[base + 16 :, :] = spread[1].astype(jnp.bfloat16)
    return (spread[0] + spread[1]).astype(jnp.bfloat16)


def solve(system, sides_width):
    lines = lax.broadcasted_iota(jnp.int32, (16, LANES), 0)
    columns = [
        jnp.broadcast_to(system[:, sides_width + k : sides_width + k + 1], (16, LANES)) for k in range(TERMS)
    ]
    sides = [system[:, start : start + LANES] for start in range(0, sides_width, LANES)]
    for k in range(TERMS):
        column = columns[k]
        inverse = 1.0 / column[k : k + 1, :]

        def eliminate(block):
            pivot = block[k : k + 1, :] * inverse
            return jnp.where(lines == k, pivot, block - column * pivot)

        sides = [eliminate(block) for block in sides]
        columns = [eliminate(block) if j > k else block for j, block in enumerate(columns)]
    return jnp.concatenate([jnp.where(lines < TERMS, block, 0.0) for block in sides], axis=1)


def compose(
    tm, space, members, all_points,
    fields, calendar, events, lags, out_ref,
    xs, calendar_ref, events_ref, lags_ref, weights_ref, normal_ref, normals, left, raws, whole, spatial, parts, ordered,
    sums, got_sums, totals, got_totals, means, codes, scales, got_codes, got_scales,
    x_sems, in_sems, n_send, n_recv, m_send, m_recv, t_send, t_recv, c_send, c_recv, s_send, s_recv,
):
    chunks, days = xs.shape[0], xs.shape[1]
    depth = weights_ref.shape[1]
    count_rows = weights_ref.shape[0] - 32
    rows = count_rows // tm
    types = events_ref.shape[0]
    lag_count = lags_ref.shape[0]
    maps = types * lag_count
    me = lax.axis_index("tm")
    here = lax.axis_index("space")
    stages = tm.bit_length() - 1

    def load(c):
        return pltpu.make_async_copy(
            fields.at[:, :, pl.ds(pl.multiple_of(c * CHUNK, CHUNK), CHUNK)], xs.at[c], x_sems.at[c]
        )

    barrier = pltpu.get_barrier_semaphore()
    for i in range(1, tm):
        pl.semaphore_signal(barrier, inc=1, device_id={"tm": lax.rem(me + i, tm)})
    for i in range(1, space):
        pl.semaphore_signal(barrier, inc=1, device_id={"space": lax.rem(here + i, space)})
    load_events = pltpu.make_async_copy(events, events_ref, in_sems.at[0])
    load_calendar = pltpu.make_async_copy(calendar, calendar_ref, in_sems.at[1])
    load_lags = pltpu.make_async_copy(lags, lags_ref, in_sems.at[2])
    load_events.start()
    load_calendar.start()
    load_lags.start()
    lax.fori_loop(0, chunks, lambda c, _: (load(c).start(), 0)[1], 0)

    def send_normal(i):
        return [
            pltpu.make_async_remote_copy(
                normal_ref.at[lines], normals.at[i - 1, lines], n_send.at[part, i - 1], n_recv.at[part, i - 1],
                device_id={"tm": lax.rem(me + i, tm)},
            )
            for part, lines in enumerate((pl.ds(0, 8), pl.ds(8, 8)))
        ]

    def send_sums(i):
        return pltpu.make_async_remote_copy(
            sums, got_sums.at[i - 1], m_send.at[i - 1], m_recv.at[i - 1],
            device_id={"space": lax.rem(here + i, space)},
        )

    def send_totals(i):
        return pltpu.make_async_remote_copy(
            totals, got_totals.at[i - 1], t_send.at[i - 1], t_recv.at[i - 1],
            device_id={"tm": lax.rem(me + i, tm)},
        )

    def bits_of(turn):
        return [1 << ((turn + stage) % stages) for stage in range(stages)]

    def leaving(turn, stage):
        bits = bits_of(turn)
        return [
            apart for apart in range(1, tm)
            if apart & bits[stage] and not any(apart & bit for bit in bits[:stage])
        ]

    def first_slot(stage):
        return tm - (tm >> stage)

    def send_codes(c, turn, stage):
        peer = {"tm": flip(me, bits_of(turn)[stage])}
        slots = pl.ds(first_slot(stage), tm >> (stage + 1))
        return (
            pltpu.make_async_remote_copy(
                codes.at[c, slots], got_codes.at[c, slots], c_send.at[stage, c], c_recv.at[stage, c], device_id=peer
            ),
            pltpu.make_async_remote_copy(
                scales.at[c, slots], got_scales.at[c, slots], s_send.at[stage, c], s_recv.at[stage, c], device_id=peer
            ),
        )

    load_events.wait()
    count_weights(2 * (events_ref[...] - me * days) + PAD, weights_ref, depth)
    load_calendar.wait()
    design = regressors(calendar_ref[...], weights_ref)
    first = weights_ref[:count_rows, :].reshape(types, 2 * lag_count, depth)[:, :lag_count, :].reshape(maps, depth)
    grams = weights_ref[count_rows : count_rows + 16, :]
    normal_ref[...] = jnp.concatenate(
        [lax.dot_general(design, side, NT, preferred_element_type=jnp.float32) for side in (first, grams)], axis=1
    )

    pl.semaphore_wait(barrier, tm + space - 2)
    for i in range(1, tm):
        for copy in send_normal(i):
            copy.start()

    def multiply(c, carry):
        load(c).wait()
        raws[c] = jnp.dot(weights_ref[...], xs[c].reshape(depth, CHUNK), preferred_element_type=jnp.float32)
        return carry

    ahead = -(-AHEAD // stages) * stages
    lax.fori_loop(0, ahead, multiply, 0)

    system = normal_ref[...]
    for i in range(1, tm):
        for copy in send_normal(i):
            copy.wait()
        system = system + normals[i - 1]
    fit = solve(system, maps)
    high, middle, low = [piece.astype(jnp.float32) for piece in split3(fit)]
    left[...] = jnp.transpose(jnp.concatenate([high, high, high, middle, middle, low], axis=0)).astype(jnp.bfloat16)
    spatial[...] = jnp.zeros_like(spatial)

    def grouped(body, start, stop):
        def group(g, carry):
            for turn in range(stages):
                body(start + g * stages + turn, turn)
            return carry

        assert (stop - start) % stages == 0
        lax.fori_loop(0, (stop - start) // stages, group, 0)

    def post(c, turn, stage):
        for slot, apart in enumerate(leaving(turn, stage)):
            place = first_slot(stage) + slot
            codes[c, place], scales[c, place] = encode(parts[apart, c])
        for copy in send_codes(c, turn, stage):
            copy.start()

    def collect(c, turn, stage):
        bit = bits_of(turn)[stage]
        for copy in send_codes(c, turn, stage):
            copy.wait_recv()
        for slot, apart in enumerate(leaving(turn, stage)):
            place = first_slot(stage) + slot
            parts[apart - bit, c] += decode(got_codes[c, place], got_scales[c, place])

    def anomalies(c, turn):
        seasonal = []
        for variable in range(2):
            start = count_rows + 16 * variable
            p_high, p_middle, p_low = split3(raws[c, start : start + 16, :])
            right = jnp.concatenate([p_high, p_middle, p_low, p_high, p_middle, p_high], axis=0)
            product = jnp.dot(left[...], right, preferred_element_type=jnp.float32)
            seasonal.append(product.reshape(types, 1, lag_count, CHUNK))
        seasonal = jnp.concatenate(seasonal, axis=1).reshape(count_rows, CHUNK)
        whole[...] = raws[c, :count_rows, :] - seasonal
        for apart in range(tm):
            parts[apart, c] = whole[pl.ds(pl.multiple_of(flip(me, apart) * rows, rows), rows), :]
        post(c, turn, 0)
        spatial[...] += whole[...]

    def both(c, turn):
        anomalies(c, turn)
        multiply(c + ahead, 0)

    grouped(both, 0, chunks - ahead)
    grouped(anomalies, chunks - ahead, chunks)

    ones = jnp.ones((8, CHUNK), jnp.bfloat16)
    total = jnp.zeros((8, count_rows), jnp.float32)
    for piece in split3(spatial[...]):
        total = total + lax.dot_general(ones, piece, NT, preferred_element_type=jnp.float32)
    sums[...] = total[0:1, :]
    for i in range(1, space):
        send_sums(i).start()

    half = chunks // 2

    def relay(stage):
        def body(c, turn):
            collect(c, turn, stage - 1)
            post(c, turn, stage)

        return body

    def spread_sums():
        total = sums[...]
        for i in range(1, space):
            send_sums(i).wait()
            total = total + got_sums[i - 1]
        totals[...] = total
        for i in range(1, tm):
            send_totals(i).start()

    for stage in range(1, stages):
        grouped(relay(stage), 0, half)
        if stage == 1:
            spread_sums()
        grouped(relay(stage), half, chunks)

    total = totals[...]
    for i in range(1, tm):
        send_totals(i).wait()
        total = total + got_totals[i - 1]
    means[...] = lax.dot_general(
        jnp.broadcast_to(total * (1.0 / (8 * members * all_points)), (8, count_rows)), jnp.ones((8, CHUNK), jnp.float32),
        TN, precision=lax.Precision.HIGHEST, preferred_element_type=jnp.float32,
    )

    load_lags.wait()

    def gather(c, turn):
        collect(c, turn, stages - 1)
        mean = means[pl.ds(pl.multiple_of(me * rows, rows), rows), :]
        value = parts[0, c] * (1.0 / members) - mean
        ordered[...] = value
        columns = pl.ds(pl.multiple_of(c * CHUNK, CHUNK), CHUNK)
        for lag in range(lag_count):
            shift = lags_ref[lag]
            for kind in range(types // tm):
                for variable in range(2):
                    line = pl.ds((2 * kind + variable) * lag_count + shift, 1)
                    out_ref[kind, lag, variable : variable + 1, columns] = ordered[line, :]

    grouped(gather, 0, chunks)

    def sent(c, turn):
        for stage in range(stages):
            for copy in send_codes(c, turn, stage):
                copy.wait_send()

    grouped(sent, 0, chunks)


def shards(tm, space, fields, calendar_day, events, lag_offsets):
    types, members = events.shape
    lag_count = lag_offsets.shape[0]
    days, variables, points = fields.shape
    depth = variables * days
    count_rows = types * lag_count * variables
    rows = count_rows // tm
    chunks = points // CHUNK
    stages = tm.bit_length() - 1
    dma = pltpu.SemaphoreType.DMA
    vmem = pltpu.VMEM
    f32, bf16 = jnp.float32, jnp.bfloat16
    shape = (types // tm, lag_count, variables, points)
    in_hbm = [
        pltpu.with_memory_space_constraint(value, pltpu.HBM)
        for value in (calendar_day.reshape(days // LANES, LANES), events, lag_offsets)
    ]
    return pl.pallas_call(
        functools.partial(compose, tm, space, members, points * space),
        out_shape=jax.ShapeDtypeStruct(shape, f32),
        in_specs=[pl.BlockSpec(memory_space=pltpu.HBM)] * 4,
        out_specs=pl.BlockSpec(memory_space=vmem),
        scratch_shapes=[
            vmem((chunks, days, variables, CHUNK), bf16),
            vmem((days // LANES, LANES), jnp.int32),
            vmem((types, members), jnp.int32),
            pltpu.SMEM((lag_count,), jnp.int32),
            vmem((count_rows + 32, depth), bf16),
            vmem((16, types * lag_count + 16), f32),
            vmem((tm - 1, 16, types * lag_count + 16), f32),
            vmem((types * lag_count, 96), bf16),
            vmem((chunks, count_rows + 32, CHUNK), f32),
            vmem((count_rows, CHUNK), f32),
            vmem((count_rows, CHUNK), f32),
            vmem((tm, chunks, rows, CHUNK), f32),
            vmem((rows, CHUNK), f32),
            vmem((1, count_rows), f32),
            vmem((space - 1, 1, count_rows), f32),
            vmem((1, count_rows), f32),
            vmem((tm - 1, 1, count_rows), f32),
            vmem((count_rows, CHUNK), f32),
            vmem((chunks, tm - 1, rows, CHUNK), jnp.int16),
            vmem((chunks, tm - 1, 1, CHUNK), f32),
            vmem((chunks, tm - 1, rows, CHUNK), jnp.int16),
            vmem((chunks, tm - 1, 1, CHUNK), f32),
            dma((chunks,)), dma((3,)),
            dma((2, tm - 1)), dma((2, tm - 1)),
            dma((space - 1,)), dma((space - 1,)),
            dma((tm - 1,)), dma((tm - 1,)),
            dma((stages, chunks)), dma((stages, chunks)), dma((stages, chunks)), dma((stages, chunks)),
        ],
        compiler_params=pltpu.CompilerParams(
            collective_id=0, has_side_effects=True, vmem_limit_bytes=52 * 2**20
        ),
        name="compose",
    )(fields, *in_hbm)


def solution(mesh):
    return jax.shard_map(
        functools.partial(shards, mesh.shape["tm"], mesh.shape["space"]),
        mesh=mesh,
        in_specs=(P("tm", None, "space"), P("tm"), P(), P()),
        out_specs=P("tm", None, None, "space"),
        check_vma=False,
    )
```

```python
import functools

import jax
import jax.numpy as jnp
from jax import lax
from jax.experimental import pallas as pl
from jax.experimental.pallas import tpu as pltpu
from jax.sharding import PartitionSpec as P

HARMONICS = 4
TERMS = 2 * HARMONICS + 1
TWO_PI = 6.283185307179586
LANES = 128
PAD = 128
CHUNK = 256
CORES = 2
AHEAD = 4
NN = (((1,), (0,)), ((), ()))
NT = (((1,), (1,)), ((), ()))
TN = (((0,), (0,)), ((), ()))


def split3(value):
    high = value.astype(jnp.bfloat16)
    rest = value - high.astype(jnp.float32)
    middle = rest.astype(jnp.bfloat16)
    low = (rest - middle.astype(jnp.float32)).astype(jnp.bfloat16)
    return high, middle, low


def encode(part):
    top = jnp.max(jnp.abs(part), axis=0, keepdims=True)
    factor = jnp.where(top > 0.0, 32767.0 / jnp.where(top > 0.0, top, 1.0), 0.0)
    return jnp.round(part * factor).astype(jnp.int32).astype(jnp.int16), top * (1.0 / 32767.0)


def decode(codes, scale):
    return codes.astype(jnp.int32).astype(jnp.float32) * scale


def flip(index, bits):
    bit = 1
    flipped = index
    while bit <= bits:
        if bits & bit:
            flipped = flipped + bit - 2 * bit * lax.rem(lax.div(index, bit), 2)
        bit *= 2
    return flipped


def ones_where(condition):
    return jnp.where(condition, 1.0, 0.0).astype(jnp.bfloat16)


def count_weights(places, weights_ref, depth):
    types, members = places.shape
    lag_count = (weights_ref.shape[0] - 32) // (2 * types)
    tiles = (depth + PAD) // LANES
    upper = lax.shift_right_arithmetic(places, 7)
    lower = lax.bitwise_and(places, LANES - 1)
    tile_lines = lax.broadcasted_iota(jnp.int32, (-(-tiles // 8) * 8, members), 0)
    lane_lines = lax.broadcasted_iota(jnp.int32, (LANES, members), 0)
    for kind in range(types):
        in_tile = ones_where(upper[kind : kind + 1, :] == tile_lines)
        in_lane = ones_where(lower[kind : kind + 1, :] == lane_lines)
        histogram = lax.dot_general(in_tile, in_lane, NT, preferred_element_type=jnp.float32)
        wide = jnp.concatenate(
            [jnp.broadcast_to(histogram[tile : tile + 1, :], (lag_count, LANES)) for tile in range(tiles)], axis=1
        )
        for variable in range(2):
            rolled = pltpu.roll(wide, variable, 1, stride=2, stride_axis=0)
            start = (2 * kind + variable) * lag_count
            weights_ref[start : start + lag_count, :] = rolled[:, PAD:].astype(jnp.bfloat16)


def regressors(calendar, weights_ref):
    phase = calendar.astype(jnp.float32) * (TWO_PI / 365.25)
    cosines, sines = [jnp.cos(phase)], [jnp.sin(phase)]
    for order in range(2, HARMONICS + 1):
        a, b = order // 2 - 1, order - order // 2 - 1
        cosines.append(cosines[a] * cosines[b] - sines[a] * sines[b])
        sines.append(sines[a] * cosines[b] + cosines[a] * sines[b])
    terms = [jnp.ones_like(phase)]
    for order in range(HARMONICS):
        terms += [cosines[order], sines[order]]
    tiles = calendar.shape[0]
    line = lax.broadcasted_iota(jnp.int32, (16, LANES), 0)
    blocks = []
    for tile in range(tiles):
        block = jnp.zeros((16, LANES), jnp.float32)
        for term, values in enumerate(terms):
            block = jnp.where(line == term, values[tile : tile + 1, :], block)
        blocks.append(block)
    stacked = jnp.concatenate(blocks, axis=0).astype(jnp.bfloat16)
    day = lax.broadcasted_iota(jnp.int32, (LANES, 2 * LANES), 0)
    place = lax.broadcasted_iota(jnp.int32, (LANES, 2 * LANES), 1)
    first = ones_where(place == 2 * day)
    second = ones_where(place == 2 * day + 1)
    base = weights_ref.shape[0] - 32
    spread = []
    for matrix in (first, second):
        wide = jnp.dot(stacked, matrix, preferred_element_type=jnp.float32)
        spread.append(jnp.concatenate([wide[16 * tile : 16 * tile + 16, :] for tile in range(tiles)], axis=1))
    weights_ref[base : base + 16, :] = spread[0].astype(jnp.bfloat16)
    weights_ref[base + 16 :, :] = spread[1].astype(jnp.bfloat16)
    return (spread[0] + spread[1]).astype(jnp.bfloat16)


def solve(system, sides_width):
    lines = lax.broadcasted_iota(jnp.int32, (16, LANES), 0)
    columns = [
        jnp.broadcast_to(system[:, sides_width + k : sides_width + k + 1], (16, LANES)) for k in range(TERMS)
    ]
    sides = [system[:, start : start + LANES] for start in range(0, sides_width, LANES)]
    for k in range(TERMS):
        column = columns[k]
        inverse = 1.0 / column[k : k + 1, :]

        def eliminate(block):
            pivot = block[k : k + 1, :] * inverse
            return jnp.where(lines == k, pivot, block - column * pivot)

        sides = [eliminate(block) for block in sides]
        columns = [eliminate(block) if j > k else block for j, block in enumerate(columns)]
    return jnp.concatenate([jnp.where(lines < TERMS, block, 0.0) for block in sides], axis=1)


def compose(
    tm, space, members, all_points,
    fields, calendar, events, lags, out_ref,
    xs, calendar_ref, events_ref, lags_ref, weights_ref, normal_ref, normals, left, raws, whole, spatial, parts, ordered,
    sums, got_sums, totals, got_totals, means, codes, scales, got_codes, got_scales,
    ready, x_sems, in_sems, n_send, n_recv, m_send, m_recv, t_send, t_recv, c_send, c_recv, s_send, s_recv,
):
    chunks, days = xs.shape[0], xs.shape[1]
    depth = weights_ref.shape[1]
    count_rows = weights_ref.shape[0] - 32
    rows = count_rows // tm
    types = events_ref.shape[0]
    lag_count = lags_ref.shape[0]
    maps = types * lag_count
    me = lax.axis_index("tm")
    here = lax.axis_index("space")
    stages = tm.bit_length() - 1

    def load(c):
        return pltpu.make_async_copy(
            fields.at[:, :, pl.ds(pl.multiple_of(c * CHUNK, CHUNK), CHUNK)], xs.at[c], x_sems.at[c]
        )

    barrier = pltpu.get_barrier_semaphore()
    for i in range(1, tm):
        pl.semaphore_signal(barrier, inc=1, device_id={"tm": lax.rem(me + i, tm)})
    chip, side, line = lax.div(here, CORES), lax.rem(here, CORES), space // CORES

    def greet(place, core):
        pl.semaphore_signal(barrier, inc=1, device_id={"space": place * CORES + core})

    def inform(way, place):
        pl.semaphore_signal(ready.at[way], inc=1, device_id={"space": place * CORES + side})

    for i in range(1, CORES):
        greet(chip, lax.rem(side + i, CORES))

    @pl.when(chip > 0)
    def _():
        for core in range(CORES):
            greet(chip - 1, core)

    @pl.when(chip < line - 1)
    def _():
        for core in range(CORES):
            greet(chip + 1, core)

    greeted = lax.min(chip, 1) + lax.min(line - 1 - chip, 1)
    load_events = pltpu.make_async_copy(events, events_ref, in_sems.at[0])
    load_calendar = pltpu.make_async_copy(calendar, calendar_ref, in_sems.at[1])
    load_lags = pltpu.make_async_copy(lags, lags_ref, in_sems.at[2])
    load_events.start()
    load_calendar.start()
    load_lags.start()
    lax.fori_loop(0, chunks, lambda c, _: (load(c).start(), 0)[1], 0)

    def send_normal(i):
        return [
            pltpu.make_async_remote_copy(
                normal_ref.at[lines], normals.at[i - 1, lines], n_send.at[part, i - 1], n_recv.at[part, i - 1],
                device_id={"tm": lax.rem(me + i, tm)},
            )
            for part, lines in enumerate((pl.ds(0, 8), pl.ds(8, 8)))
        ]

    def send_sums(i):
        return pltpu.make_async_remote_copy(
            sums, got_sums.at[i - 1], m_send.at[i - 1], m_recv.at[i - 1],
            device_id={"space": lax.rem(here + i, space)},
        )

    def send_totals(i):
        return pltpu.make_async_remote_copy(
            totals, got_totals.at[i - 1], t_send.at[i - 1], t_recv.at[i - 1],
            device_id={"tm": lax.rem(me + i, tm)},
        )

    def bits_of(turn):
        return [1 << ((turn + stage) % stages) for stage in range(stages)]

    def leaving(turn, stage):
        bits = bits_of(turn)
        return [
            apart for apart in range(1, tm)
            if apart & bits[stage] and not any(apart & bit for bit in bits[:stage])
        ]

    def first_slot(stage):
        return tm - (tm >> stage)

    def send_codes(c, turn, stage):
        peer = {"tm": flip(me, bits_of(turn)[stage])}
        slots = pl.ds(first_slot(stage), tm >> (stage + 1))
        return (
            pltpu.make_async_remote_copy(
                codes.at[c, slots], got_codes.at[c, slots], c_send.at[stage, c], c_recv.at[stage, c], device_id=peer
            ),
            pltpu.make_async_remote_copy(
                scales.at[c, slots], got_scales.at[c, slots], s_send.at[stage, c], s_recv.at[stage, c], device_id=peer
            ),
        )

    load_events.wait()
    count_weights(2 * (events_ref[...] - me * days) + PAD, weights_ref, depth)
    load_calendar.wait()
    design = regressors(calendar_ref[...], weights_ref)
    first = weights_ref[:count_rows, :].reshape(types, 2 * lag_count, depth)[:, :lag_count, :].reshape(maps, depth)
    grams = weights_ref[count_rows : count_rows + 16, :]
    normal_ref[...] = jnp.concatenate(
        [lax.dot_general(design, side, NT, preferred_element_type=jnp.float32) for side in (first, grams)], axis=1
    )

    pl.semaphore_wait(barrier, tm - 1 + CORES - 1 + CORES * greeted)
    if line > 2:
        pl.when(chip == 1)(lambda: inform(0, chip + 1))
        pl.when(chip == line - 2)(lambda: inform(1, chip - 1))
    for i in range(1, tm):
        for copy in send_normal(i):
            copy.start()

    def multiply(c, carry):
        load(c).wait()
        raws[c] = jnp.dot(weights_ref[...], xs[c].reshape(depth, CHUNK), preferred_element_type=jnp.float32)
        return carry

    ahead = -(-AHEAD // stages) * stages
    lax.fori_loop(0, ahead, multiply, 0)

    system = normal_ref[...]
    for i in range(1, tm):
        for copy in send_normal(i):
            copy.wait()
        system = system + normals[i - 1]
    if line > 3:

        @pl.when(jnp.logical_and(chip >= 2, chip < line - 1))
        def _():
            pl.semaphore_wait(ready.at[0], 1)
            inform(0, chip + 1)

        @pl.when(jnp.logical_and(chip <= line - 3, chip > 0))
        def _():
            pl.semaphore_wait(ready.at[1], 1)
            inform(1, chip - 1)

    fit = solve(system, maps)
    high, middle, low = [piece.astype(jnp.float32) for piece in split3(fit)]
    left[...] = jnp.transpose(jnp.concatenate([high, high, high, middle, middle, low], axis=0)).astype(jnp.bfloat16)
    spatial[...] = jnp.zeros_like(spatial)

    def grouped(body, start, stop):
        def group(g, carry):
            for turn in range(stages):
                body(start + g * stages + turn, turn)
            return carry

        assert (stop - start) % stages == 0
        lax.fori_loop(0, (stop - start) // stages, group, 0)

    def post(c, turn, stage):
        for slot, apart in enumerate(leaving(turn, stage)):
            place = first_slot(stage) + slot
            codes[c, place], scales[c, place] = encode(parts[apart, c])
        for copy in send_codes(c, turn, stage):
            copy.start()

    def collect(c, turn, stage):
        bit = bits_of(turn)[stage]
        for copy in send_codes(c, turn, stage):
            copy.wait_recv()
        for slot, apart in enumerate(leaving(turn, stage)):
            place = first_slot(stage) + slot
            parts[apart - bit, c] += decode(got_codes[c, place], got_scales[c, place])

    def anomalies(c, turn):
        seasonal = []
        for variable in range(2):
            start = count_rows + 16 * variable
            p_high, p_middle, p_low = split3(raws[c, start : start + 16, :])
            right = jnp.concatenate([p_high, p_middle, p_low, p_high, p_middle, p_high], axis=0)
            product = jnp.dot(left[...], right, preferred_element_type=jnp.float32)
            seasonal.append(product.reshape(types, 1, lag_count, CHUNK))
        seasonal = jnp.concatenate(seasonal, axis=1).reshape(count_rows, CHUNK)
        whole[...] = raws[c, :count_rows, :] - seasonal
        for apart in range(tm):
            parts[apart, c] = whole[pl.ds(pl.multiple_of(flip(me, apart) * rows, rows), rows), :]
        post(c, turn, 0)
        spatial[...] += whole[...]

    def both(c, turn):
        anomalies(c, turn)
        multiply(c + ahead, 0)

    grouped(both, 0, chunks - ahead)
    grouped(anomalies, chunks - ahead, chunks)

    ones = jnp.ones((8, CHUNK), jnp.bfloat16)
    total = jnp.zeros((8, count_rows), jnp.float32)
    for piece in split3(spatial[...]):
        total = total + lax.dot_general(ones, piece, NT, preferred_element_type=jnp.float32)
    sums[...] = total[0:1, :]
    if line > 2:
        pl.when(chip == line - 1)(lambda: pl.semaphore_wait(ready.at[0], 1))
        pl.when(chip == 0)(lambda: pl.semaphore_wait(ready.at[1], 1))
    for i in range(1, space):
        send_sums(i).start()

    half = chunks // 2

    def relay(stage):
        def body(c, turn):
            collect(c, turn, stage - 1)
            post(c, turn, stage)

        return body

    def spread_sums():
        total = sums[...]
        for i in range(1, space):
            send_sums(i).wait()
            total = total + got_sums[i - 1]
        totals[...] = total
        for i in range(1, tm):
            send_totals(i).start()

    for stage in range(1, stages):
        grouped(relay(stage), 0, half)
        if stage == 1:
            spread_sums()
        grouped(relay(stage), half, chunks)

    total = totals[...]
    for i in range(1, tm):
        send_totals(i).wait()
        total = total + got_totals[i - 1]
    means[...] = lax.dot_general(
        jnp.broadcast_to(total * (1.0 / (8 * members * all_points)), (8, count_rows)), jnp.ones((8, CHUNK), jnp.float32),
        TN, precision=lax.Precision.HIGHEST, preferred_element_type=jnp.float32,
    )

    load_lags.wait()

    def gather(c, turn):
        collect(c, turn, stages - 1)
        mean = means[pl.ds(pl.multiple_of(me * rows, rows), rows), :]
        value = parts[0, c] * (1.0 / members) - mean
        ordered[...] = value
        columns = pl.ds(pl.multiple_of(c * CHUNK, CHUNK), CHUNK)
        for lag in range(lag_count):
            shift = lags_ref[lag]
            for kind in range(types // tm):
                for variable in range(2):
                    line = pl.ds((2 * kind + variable) * lag_count + shift, 1)
                    out_ref[kind, lag, variable : variable + 1, columns] = ordered[line, :]

    grouped(gather, 0, chunks)

    def sent(c, turn):
        for stage in range(stages):
            for copy in send_codes(c, turn, stage):
                copy.wait_send()

    grouped(sent, 0, chunks)


def shards(tm, space, fields, calendar_day, events, lag_offsets):
    types, members = events.shape
    lag_count = lag_offsets.shape[0]
    days, variables, points = fields.shape
    depth = variables * days
    count_rows = types * lag_count * variables
    rows = count_rows // tm
    chunks = points // CHUNK
    stages = tm.bit_length() - 1
    dma = pltpu.SemaphoreType.DMA
    vmem = pltpu.VMEM
    f32, bf16 = jnp.float32, jnp.bfloat16
    shape = (types // tm, lag_count, variables, points)
    in_hbm = [
        pltpu.with_memory_space_constraint(value, pltpu.HBM)
        for value in (calendar_day.reshape(days // LANES, LANES), events, lag_offsets)
    ]
    return pl.pallas_call(
        functools.partial(compose, tm, space, members, points * space),
        out_shape=jax.ShapeDtypeStruct(shape, f32),
        in_specs=[pl.BlockSpec(memory_space=pltpu.HBM)] * 4,
        out_specs=pl.BlockSpec(memory_space=vmem),
        scratch_shapes=[
            vmem((chunks, days, variables, CHUNK), bf16),
            vmem((days // LANES, LANES), jnp.int32),
            vmem((types, members), jnp.int32),
            pltpu.SMEM((lag_count,), jnp.int32),
            vmem((count_rows + 32, depth), bf16),
            vmem((16, types * lag_count + 16), f32),
            vmem((tm - 1, 16, types * lag_count + 16), f32),
            vmem((types * lag_count, 96), bf16),
            vmem((chunks, count_rows + 32, CHUNK), f32),
            vmem((count_rows, CHUNK), f32),
            vmem((count_rows, CHUNK), f32),
            vmem((tm, chunks, rows, CHUNK), f32),
            vmem((rows, CHUNK), f32),
            vmem((1, count_rows), f32),
            vmem((space - 1, 1, count_rows), f32),
            vmem((1, count_rows), f32),
            vmem((tm - 1, 1, count_rows), f32),
            vmem((count_rows, CHUNK), f32),
            vmem((chunks, tm - 1, rows, CHUNK), jnp.int16),
            vmem((chunks, tm - 1, 1, CHUNK), f32),
            vmem((chunks, tm - 1, rows, CHUNK), jnp.int16),
            vmem((chunks, tm - 1, 1, CHUNK), f32),
            pltpu.SemaphoreType.REGULAR((2,)),
            dma((chunks,)), dma((3,)),
            dma((2, tm - 1)), dma((2, tm - 1)),
            dma((space - 1,)), dma((space - 1,)),
            dma((tm - 1,)), dma((tm - 1,)),
            dma((stages, chunks)), dma((stages, chunks)), dma((stages, chunks)), dma((stages, chunks)),
        ],
        compiler_params=pltpu.CompilerParams(
            collective_id=0, has_side_effects=True, vmem_limit_bytes=52 * 2**20
        ),
        name="compose",
    )(fields, *in_hbm)


def solution(mesh):
    return jax.shard_map(
        functools.partial(shards, mesh.shape["tm"], mesh.shape["space"]),
        mesh=mesh,
        in_specs=(P("tm", None, "space"), P("tm"), P(), P()),
        out_specs=P("tm", None, None, "space"),
        check_vma=False,
    )
```

```python
import functools

import jax
import jax.numpy as jnp
from jax import lax
from jax.experimental import pallas as pl
from jax.experimental.pallas import tpu as pltpu
from jax.sharding import PartitionSpec as P

HARMONICS = 4
TERMS = 2 * HARMONICS + 1
TWO_PI = 6.283185307179586
LANES = 128
PAD = 128
CHUNK = 256
AHEAD = 2
TURNS = 2
NN = (((1,), (0,)), ((), ()))
NT = (((1,), (1,)), ((), ()))
TN = (((0,), (0,)), ((), ()))


def split3(value):
    high = value.astype(jnp.bfloat16)
    rest = value - high.astype(jnp.float32)
    middle = rest.astype(jnp.bfloat16)
    low = (rest - middle.astype(jnp.float32)).astype(jnp.bfloat16)
    return high, middle, low


def encode(part):
    top = jnp.max(jnp.abs(part), axis=0, keepdims=True)
    factor = jnp.where(top > 0.0, 32767.0 / jnp.where(top > 0.0, top, 1.0), 0.0)
    return jnp.round(part * factor).astype(jnp.int32).astype(jnp.int16), top * (1.0 / 32767.0)


def decode(codes, scale):
    return codes.astype(jnp.int32).astype(jnp.float32) * scale


def flip(index, bits):
    bit = 1
    flipped = index
    while bit <= bits:
        if bits & bit:
            flipped = flipped + bit - 2 * bit * lax.rem(lax.div(index, bit), 2)
        bit *= 2
    return flipped


def ones_where(condition):
    return jnp.where(condition, 1.0, 0.0).astype(jnp.bfloat16)


def histograms(places, tiles):
    members = places.shape[1]
    upper = lax.shift_right_arithmetic(places, 7)
    lower = lax.bitwise_and(places, LANES - 1)
    tile_lines = lax.broadcasted_iota(jnp.int32, (-(-tiles // 8) * 8, members), 0)
    lane_lines = lax.broadcasted_iota(jnp.int32, (LANES, members), 0)
    for kind in range(places.shape[0]):
        in_tile = ones_where(upper[kind : kind + 1, :] == tile_lines)
        in_lane = ones_where(lower[kind : kind + 1, :] == lane_lines)
        yield lax.dot_general(in_tile, in_lane, NT, preferred_element_type=jnp.float32)


def widen(histogram, tiles, lines):
    return jnp.concatenate(
        [jnp.broadcast_to(histogram[tile : tile + 1, :], (lines, LANES)) for tile in range(tiles)], axis=1
    )


def count_weights(places, weights_ref, lag_count):
    tiles = (weights_ref.shape[1] + PAD) // LANES
    for kind, histogram in enumerate(histograms(places, tiles)):
        wide = widen(histogram, tiles, lag_count)
        for variable in range(2):
            rolled = pltpu.roll(wide, variable, 1, stride=2, stride_axis=0)
            start = (2 * kind + variable) * lag_count
            weights_ref[start : start + lag_count, :] = rolled[:, PAD:].astype(jnp.bfloat16)


def count_days(places, counts_ref, lag_count):
    tiles = (counts_ref.shape[1] + PAD) // LANES
    for kind, histogram in enumerate(histograms(places, tiles)):
        rolled = pltpu.roll(widen(histogram, tiles, lag_count), 0, 1, stride=1, stride_axis=0)
        counts_ref[kind * lag_count : (kind + 1) * lag_count, :] = rolled[:, PAD:].astype(jnp.bfloat16)


def regressors(calendar):
    phase = calendar.astype(jnp.float32) * (TWO_PI / 365.25)
    cosines, sines = [jnp.cos(phase)], [jnp.sin(phase)]
    for order in range(2, HARMONICS + 1):
        a, b = order // 2 - 1, order - order // 2 - 1
        cosines.append(cosines[a] * cosines[b] - sines[a] * sines[b])
        sines.append(sines[a] * cosines[b] + cosines[a] * sines[b])
    terms = [jnp.ones_like(phase)]
    for order in range(HARMONICS):
        terms += [cosines[order], sines[order]]
    line = lax.broadcasted_iota(jnp.int32, (16, LANES), 0)
    blocks = []
    for tile in range(calendar.shape[0]):
        block = jnp.zeros((16, LANES), jnp.float32)
        for term, values in enumerate(terms):
            block = jnp.where(line == term, values[tile : tile + 1, :], block)
        blocks.append(block)
    return blocks


def own_regressors(calendar, weights_ref):
    tiles = calendar.shape[0]
    stacked = jnp.concatenate(regressors(calendar), axis=0).astype(jnp.bfloat16)
    day = lax.broadcasted_iota(jnp.int32, (LANES, 2 * LANES), 0)
    place = lax.broadcasted_iota(jnp.int32, (LANES, 2 * LANES), 1)
    start = weights_ref.shape[0] - 32
    for variable in range(2):
        spread = jnp.dot(stacked, ones_where(place == 2 * day + variable), preferred_element_type=jnp.float32)
        lines = jnp.concatenate([spread[16 * tile : 16 * tile + 16, :] for tile in range(tiles)], axis=1)
        weights_ref[start + 16 * variable : start + 16 * variable + 16, :] = lines.astype(jnp.bfloat16)


def solve(system, sides_width):
    lines = lax.broadcasted_iota(jnp.int32, (16, LANES), 0)
    columns = [
        jnp.broadcast_to(system[:, sides_width + k : sides_width + k + 1], (16, LANES)) for k in range(TERMS)
    ]
    sides = [system[:, start : start + LANES] for start in range(0, sides_width, LANES)]
    for k in range(TERMS):
        column = columns[k]
        inverse = 1.0 / column[k : k + 1, :]

        def eliminate(block):
            pivot = block[k : k + 1, :] * inverse
            return jnp.where(lines == k, pivot, block - column * pivot)

        sides = [eliminate(block) for block in sides]
        columns = [eliminate(block) if j > k else block for j, block in enumerate(columns)]
    return jnp.concatenate([jnp.where(lines < TERMS, block, 0.0) for block in sides], axis=1)


def compose(
    tm, space, members, all_points,
    fields, calendar, events, lags, out_ref,
    xs, calendars, events_ref, lags_ref, weights_ref, counts_ref, left, raws, whole, spatial, parts, order,
    sums, got_sums, totals, got_totals, means, codes, scales, got_codes, got_scales,
    ready, x_sems, in_sems, n_send, n_recv, m_send, m_recv, t_send, t_recv, c_send, c_recv, s_send, s_recv,
):
    chunks, days = xs.shape[0], xs.shape[1]
    depth = weights_ref.shape[1]
    count_rows = weights_ref.shape[0] - 32
    rows = count_rows // tm
    types = events_ref.shape[0]
    lag_count = lags_ref.shape[0]
    maps = types * lag_count
    me = lax.axis_index("tm")
    here = lax.axis_index("space")
    stages = tm.bit_length() - 1

    def load(c):
        return pltpu.make_async_copy(
            fields.at[:, :, pl.ds(pl.multiple_of(c * CHUNK, CHUNK), CHUNK)], xs.at[c], x_sems.at[c]
        )

    barrier = pltpu.get_barrier_semaphore()
    for i in range(1, tm):
        pl.semaphore_signal(barrier, inc=1, device_id={"tm": lax.rem(me + i, tm)})

    def greet(place, carry):
        pl.semaphore_signal(barrier, inc=1, device_id={"space": place})
        return carry

    def answer(place, carry):
        pl.semaphore_signal(ready, inc=1, device_id={"space": place})
        return carry

    lax.fori_loop(here + 1, space, greet, 0)
    load_events = pltpu.make_async_copy(events, events_ref, in_sems.at[0])
    tiles = days // LANES
    own = pl.ds(pl.multiple_of(me * tiles, tiles), tiles)
    load_calendar = pltpu.make_async_copy(calendar, calendars.at[own], in_sems.at[1])
    load_lags = pltpu.make_async_copy(lags, lags_ref, in_sems.at[2])
    load_calendar.start()
    load_events.start()
    load_lags.start()
    lax.fori_loop(0, chunks, lambda c, _: (load(c).start(), 0)[1], 0)

    def send_calendar(i):
        return pltpu.make_async_remote_copy(
            calendars.at[own], calendars.at[own], n_send.at[i - 1], n_recv.at[i - 1],
            device_id={"tm": lax.rem(me + i, tm)},
        )

    def send_sums(i):
        return pltpu.make_async_remote_copy(
            sums, got_sums.at[i - 1], m_send.at[i - 1], m_recv.at[i - 1],
            device_id={"space": lax.rem(here + i, space)},
        )

    def send_totals(i):
        return pltpu.make_async_remote_copy(
            totals, got_totals.at[i - 1], t_send.at[i - 1], t_recv.at[i - 1],
            device_id={"tm": lax.rem(me + i, tm)},
        )

    def bits_of(turn):
        return [1 << ((turn * stages // TURNS + stage) % stages) for stage in range(stages)]

    half_rows = rows // TURNS

    def leaving(turn, stage):
        bits = bits_of(turn)
        return [
            apart for apart in range(1, tm)
            if apart & bits[stage] and not any(apart & bit for bit in bits[:stage])
        ]

    def first_slot(stage):
        return tm - (tm >> stage)

    def send_codes(c, turn, stage):
        peer = {"tm": flip(me, bits_of(turn)[stage])}
        slots = pl.ds(first_slot(stage), tm >> (stage + 1))
        return (
            pltpu.make_async_remote_copy(
                codes.at[c, turn, slots], got_codes.at[c, turn, slots],
                c_send.at[stage, turn, c], c_recv.at[stage, turn, c], device_id=peer,
            ),
            pltpu.make_async_remote_copy(
                scales.at[c, turn, slots], got_scales.at[c, turn, slots],
                s_send.at[stage, turn, c], s_recv.at[stage, turn, c], device_id=peer,
            ),
        )

    load_calendar.wait()
    pl.semaphore_wait(barrier, tm - 1 + here)
    for i in range(1, tm):
        send_calendar(i).start()
    lax.fori_loop(0, here, answer, 0)
    load_events.wait()
    count_weights(2 * (events_ref[...] - me * days) + PAD, weights_ref, lag_count)
    count_days(events_ref[...] + PAD, counts_ref, lag_count)
    own_regressors(calendars[own, :], weights_ref)

    def multiply(c):
        load(c).wait()
        raws[c] = jnp.dot(weights_ref[...], xs[c].reshape(depth, CHUNK), preferred_element_type=jnp.float32)

    def each(body, start, stop):
        lax.fori_loop(start, stop, lambda c, _: (body(c), 0)[1], 0)

    each(multiply, 0, AHEAD)

    for i in range(1, tm):
        send_calendar(i).wait()
    design = jnp.concatenate(regressors(calendars[...]), axis=1).astype(jnp.bfloat16)
    system = jnp.concatenate(
        [
            lax.dot_general(design, side, NT, preferred_element_type=jnp.float32)
            for side in (counts_ref[...], design)
        ],
        axis=1,
    )
    fit = solve(system, maps)
    high, middle, low = [piece.astype(jnp.float32) for piece in split3(fit)]
    left[...] = jnp.transpose(jnp.concatenate([high, high, high, middle, middle, low], axis=0)).astype(jnp.bfloat16)
    spatial[...] = jnp.zeros_like(spatial)

    def post(c, stage):
        for turn in range(TURNS):
            lines = slice(turn * half_rows, (turn + 1) * half_rows)
            for slot, apart in enumerate(leaving(turn, stage)):
                place = first_slot(stage) + slot
                codes[c, turn, place], scales[c, turn, place] = encode(parts[apart, c, lines])
            for copy in send_codes(c, turn, stage):
                copy.start()

    def collect(c, stage):
        for turn in range(TURNS):
            bit = bits_of(turn)[stage]
            lines = slice(turn * half_rows, (turn + 1) * half_rows)
            for copy in send_codes(c, turn, stage):
                copy.wait_recv()
            for slot, apart in enumerate(leaving(turn, stage)):
                place = first_slot(stage) + slot
                parts[apart - bit, c, lines] += decode(got_codes[c, turn, place], got_scales[c, turn, place])

    def anomalies(c):
        seasonal = []
        for variable in range(2):
            start = count_rows + 16 * variable
            p_high, p_middle, p_low = split3(raws[c, start : start + 16, :])
            right = jnp.concatenate([p_high, p_middle, p_low, p_high, p_middle, p_high], axis=0)
            product = jnp.dot(left[...], right, preferred_element_type=jnp.float32)
            seasonal.append(product.reshape(types, 1, lag_count, CHUNK))
        seasonal = jnp.concatenate(seasonal, axis=1).reshape(count_rows, CHUNK)
        whole[...] = raws[c, :count_rows, :] - seasonal
        for apart in range(tm):
            parts[apart, c] = whole[pl.ds(pl.multiple_of(flip(me, apart) * rows, rows), rows), :]
        post(c, 0)
        spatial[...] += whole[...]

    def both(c):
        anomalies(c)
        multiply(c + AHEAD)

    each(both, 0, chunks - AHEAD)
    each(anomalies, chunks - AHEAD, chunks)

    ones = jnp.ones((8, CHUNK), jnp.bfloat16)
    total = jnp.zeros((8, count_rows), jnp.float32)
    for piece in split3(spatial[...]):
        total = total + lax.dot_general(ones, piece, NT, preferred_element_type=jnp.float32)
    sums[...] = total[0:1, :]

    @pl.when(here < space - 1)
    def _():
        pl.semaphore_wait(ready, space - 1 - here)

    for i in range(1, space):
        send_sums(i).start()

    load_lags.wait()
    target = lax.broadcasted_iota(jnp.int32, (rows, rows), 0)
    source = lax.broadcasted_iota(jnp.int32, (rows, rows), 1)
    group = 2 * lag_count
    assert group & (group - 1) == 0
    inside = lax.bitwise_and(target, group - 1)
    base = target - inside + lax.bitwise_and(target, 1) * lag_count
    place = lax.shift_right_logical(inside, 1)
    wanted = base
    for lag in range(lag_count):
        wanted = jnp.where(place == lag, base + lags_ref[lag], wanted)
    order[...] = ones_where(source == wanted)

    half = chunks // 2

    def relay(stage):
        def body(c):
            collect(c, stage - 1)
            post(c, stage)

        return body

    def spread_sums():
        total = sums[...]
        for i in range(1, space):
            send_sums(i).wait()
            total = total + got_sums[i - 1]
        totals[...] = total
        for i in range(1, tm):
            send_totals(i).start()

    for stage in range(1, stages):
        each(relay(stage), 0, half)
        if stage == 1:
            spread_sums()
        each(relay(stage), half, chunks)

    total = totals[...]
    for i in range(1, tm):
        send_totals(i).wait()
        total = total + got_totals[i - 1]
    means[...] = lax.dot_general(
        jnp.broadcast_to(total * (1.0 / (8 * members * all_points)), (8, count_rows)), jnp.ones((8, CHUNK), jnp.float32),
        TN, precision=lax.Precision.HIGHEST, preferred_element_type=jnp.float32,
    )


    def gather(c):
        collect(c, stages - 1)
        mean = means[pl.ds(pl.multiple_of(me * rows, rows), rows), :]
        value = parts[0, c] * (1.0 / members) - mean
        placed = sum(jnp.dot(order[...], piece, preferred_element_type=jnp.float32) for piece in split3(value))
        columns = pl.ds(pl.multiple_of(c * CHUNK, CHUNK), CHUNK)
        out_ref[:, :, :, columns] = placed.reshape(out_ref.shape[:3] + (CHUNK,))

    each(gather, 0, chunks)

    def sent(c):
        for turn in range(TURNS):
            for stage in range(stages):
                for copy in send_codes(c, turn, stage):
                    copy.wait_send()

    each(sent, 0, chunks)


def shards(tm, space, fields, calendar_day, events, lag_offsets):
    types, members = events.shape
    lag_count = lag_offsets.shape[0]
    days, variables, points = fields.shape
    depth = variables * days
    count_rows = types * lag_count * variables
    rows = count_rows // tm
    chunks = points // CHUNK
    sent = (chunks, TURNS, tm - 1)
    copies = (tm.bit_length() - 1, TURNS, chunks)
    dma = pltpu.SemaphoreType.DMA
    vmem = pltpu.VMEM
    f32, bf16 = jnp.float32, jnp.bfloat16
    shape = (types // tm, lag_count, variables, points)
    in_hbm = [
        pltpu.with_memory_space_constraint(value, pltpu.HBM)
        for value in (calendar_day.reshape(days // LANES, LANES), events, lag_offsets)
    ]
    return pl.pallas_call(
        functools.partial(compose, tm, space, members, points * space),
        out_shape=jax.ShapeDtypeStruct(shape, f32),
        in_specs=[pl.BlockSpec(memory_space=pltpu.HBM)] * 4,
        out_specs=pl.BlockSpec(memory_space=vmem),
        scratch_shapes=[
            vmem((chunks, days, variables, CHUNK), bf16),
            vmem((tm * days // LANES, LANES), jnp.int32),
            vmem((types, members), jnp.int32),
            pltpu.SMEM((lag_count,), jnp.int32),
            vmem((count_rows + 32, depth), bf16),
            vmem((types * lag_count, tm * days), bf16),
            vmem((types * lag_count, 96), bf16),
            vmem((chunks, count_rows + 32, CHUNK), f32),
            vmem((count_rows, CHUNK), f32),
            vmem((count_rows, CHUNK), f32),
            vmem((tm, chunks, rows, CHUNK), f32),
            vmem((rows, rows), bf16),
            vmem((1, count_rows), f32),
            vmem((space - 1, 1, count_rows), f32),
            vmem((1, count_rows), f32),
            vmem((tm - 1, 1, count_rows), f32),
            vmem((count_rows, CHUNK), f32),
            vmem(sent + (rows // TURNS, CHUNK), jnp.int16),
            vmem(sent + (1, CHUNK), f32),
            vmem(sent + (rows // TURNS, CHUNK), jnp.int16),
            vmem(sent + (1, CHUNK), f32),
            pltpu.SemaphoreType.REGULAR,
            dma((chunks,)), dma((3,)),
            dma((tm - 1,)), dma((tm - 1,)),
            dma((space - 1,)), dma((space - 1,)),
            dma((tm - 1,)), dma((tm - 1,)),
            dma(copies), dma(copies), dma(copies), dma(copies),
        ],
        compiler_params=pltpu.CompilerParams(
            collective_id=0, has_side_effects=True, vmem_limit_bytes=52 * 2**20
        ),
        name="compose",
    )(fields, *in_hbm)


def solution(mesh):
    return jax.shard_map(
        functools.partial(shards, mesh.shape["tm"], mesh.shape["space"]),
        mesh=mesh,
        in_specs=(P("tm", None, "space"), P("tm"), P(), P()),
        out_specs=P("tm", None, None, "space"),
        check_vma=False,
    )
```

```python
import functools

import jax
import jax.numpy as jnp
from jax import lax
from jax.experimental import pallas as pl
from jax.experimental.pallas import tpu as pltpu
from jax.sharding import PartitionSpec as P

HARMONICS = 4
TERMS = 2 * HARMONICS + 1
TWO_PI = 6.283185307179586
LANES = 128
PAD = 128
CHUNK = 512
AHEAD = 1
TURNS = 2
NN = (((1,), (0,)), ((), ()))
NT = (((1,), (1,)), ((), ()))
TN = (((0,), (0,)), ((), ()))


def split3(value):
    high = value.astype(jnp.bfloat16)
    rest = value - high.astype(jnp.float32)
    middle = rest.astype(jnp.bfloat16)
    low = (rest - middle.astype(jnp.float32)).astype(jnp.bfloat16)
    return high, middle, low


def encode(part):
    top = jnp.max(jnp.abs(part), axis=0, keepdims=True)
    factor = jnp.where(top > 0.0, 32767.0 / jnp.where(top > 0.0, top, 1.0), 0.0)
    return jnp.round(part * factor).astype(jnp.int32).astype(jnp.int16), top * (1.0 / 32767.0)


def decode(codes, scale):
    return codes.astype(jnp.int32).astype(jnp.float32) * scale


def flip(index, bits):
    bit = 1
    flipped = index
    while bit <= bits:
        if bits & bit:
            flipped = flipped + bit - 2 * bit * lax.rem(lax.div(index, bit), 2)
        bit *= 2
    return flipped


def ones_where(condition):
    return jnp.where(condition, 1.0, 0.0).astype(jnp.bfloat16)


def histograms(places, tiles):
    members = places.shape[1]
    upper = lax.shift_right_arithmetic(places, 7)
    lower = lax.bitwise_and(places, LANES - 1)
    tile_lines = lax.broadcasted_iota(jnp.int32, (-(-tiles // 8) * 8, members), 0)
    lane_lines = lax.broadcasted_iota(jnp.int32, (LANES, members), 0)
    for kind in range(places.shape[0]):
        in_tile = ones_where(upper[kind : kind + 1, :] == tile_lines)
        in_lane = ones_where(lower[kind : kind + 1, :] == lane_lines)
        yield lax.dot_general(in_tile, in_lane, NT, preferred_element_type=jnp.float32)


def widen(histogram, tiles, lines):
    return jnp.concatenate(
        [jnp.broadcast_to(histogram[tile : tile + 1, :], (lines, LANES)) for tile in range(tiles)], axis=1
    )


def count_weights(places, weights_ref, lag_count):
    tiles = (weights_ref.shape[1] + PAD) // LANES
    for kind, histogram in enumerate(histograms(places, tiles)):
        wide = widen(histogram, tiles, lag_count)
        for variable in range(2):
            rolled = pltpu.roll(wide, variable, 1, stride=2, stride_axis=0)
            start = (2 * kind + variable) * lag_count
            weights_ref[start : start + lag_count, :] = rolled[:, PAD:].astype(jnp.bfloat16)


def count_days(places, counts_ref, lag_count):
    tiles = (counts_ref.shape[1] + PAD) // LANES
    for kind, histogram in enumerate(histograms(places, tiles)):
        rolled = pltpu.roll(widen(histogram, tiles, lag_count), 0, 1, stride=1, stride_axis=0)
        counts_ref[kind * lag_count : (kind + 1) * lag_count, :] = rolled[:, PAD:].astype(jnp.bfloat16)


def regressors(calendar):
    phase = calendar.astype(jnp.float32) * (TWO_PI / 365.25)
    cosines, sines = [jnp.cos(phase)], [jnp.sin(phase)]
    for order in range(2, HARMONICS + 1):
        a, b = order // 2 - 1, order - order // 2 - 1
        cosines.append(cosines[a] * cosines[b] - sines[a] * sines[b])
        sines.append(sines[a] * cosines[b] + cosines[a] * sines[b])
    terms = [jnp.ones_like(phase)]
    for order in range(HARMONICS):
        terms += [cosines[order], sines[order]]
    line = lax.broadcasted_iota(jnp.int32, (16, LANES), 0)
    blocks = []
    for tile in range(calendar.shape[0]):
        block = jnp.zeros((16, LANES), jnp.float32)
        for term, values in enumerate(terms):
            block = jnp.where(line == term, values[tile : tile + 1, :], block)
        blocks.append(block)
    return blocks


def own_regressors(calendar, weights_ref):
    tiles = calendar.shape[0]
    stacked = jnp.concatenate(regressors(calendar), axis=0).astype(jnp.bfloat16)
    day = lax.broadcasted_iota(jnp.int32, (LANES, 2 * LANES), 0)
    place = lax.broadcasted_iota(jnp.int32, (LANES, 2 * LANES), 1)
    start = weights_ref.shape[0] - 32
    for variable in range(2):
        spread = jnp.dot(stacked, ones_where(place == 2 * day + variable), preferred_element_type=jnp.float32)
        lines = jnp.concatenate([spread[16 * tile : 16 * tile + 16, :] for tile in range(tiles)], axis=1)
        weights_ref[start + 16 * variable : start + 16 * variable + 16, :] = lines.astype(jnp.bfloat16)


def solve(system, sides_width):
    lines = lax.broadcasted_iota(jnp.int32, (16, LANES), 0)
    columns = [
        jnp.broadcast_to(system[:, sides_width + k : sides_width + k + 1], (16, LANES)) for k in range(TERMS)
    ]
    sides = [system[:, start : start + LANES] for start in range(0, sides_width, LANES)]
    for k in range(TERMS):
        column = columns[k]
        inverse = 1.0 / column[k : k + 1, :]

        def eliminate(block):
            pivot = block[k : k + 1, :] * inverse
            return jnp.where(lines == k, pivot, block - column * pivot)

        sides = [eliminate(block) for block in sides]
        columns = [eliminate(block) if j > k else block for j, block in enumerate(columns)]
    return jnp.concatenate([jnp.where(lines < TERMS, block, 0.0) for block in sides], axis=1)


def compose(
    tm, space, members, all_points,
    fields, calendar, events, lags, out_ref,
    xs, calendars, events_ref, lags_ref, weights_ref, counts_ref, left, raws, whole, spatial, parts, order,
    sums, got_sums, totals, got_totals, means, codes, scales, got_codes, got_scales,
    ready, x_sems, in_sems, n_send, n_recv, m_send, m_recv, t_send, t_recv, c_send, c_recv, s_send, s_recv,
):
    chunks, days = xs.shape[0], xs.shape[1]
    depth = weights_ref.shape[1]
    count_rows = weights_ref.shape[0] - 32
    rows = count_rows // tm
    types = events_ref.shape[0]
    lag_count = lags_ref.shape[0]
    maps = types * lag_count
    me = lax.axis_index("tm")
    here = lax.axis_index("space")
    stages = tm.bit_length() - 1

    def load(c):
        return pltpu.make_async_copy(
            fields.at[:, :, pl.ds(pl.multiple_of(c * CHUNK, CHUNK), CHUNK)], xs.at[c], x_sems.at[c]
        )

    barrier = pltpu.get_barrier_semaphore()
    for i in range(1, tm):
        pl.semaphore_signal(barrier, inc=1, device_id={"tm": lax.rem(me + i, tm)})

    def greet(place, carry):
        pl.semaphore_signal(barrier, inc=1, device_id={"space": place})
        return carry

    def answer(place, carry):
        pl.semaphore_signal(ready, inc=1, device_id={"space": place})
        return carry

    lax.fori_loop(here + 1, space, greet, 0)
    load_events = pltpu.make_async_copy(events, events_ref, in_sems.at[0])
    tiles = days // LANES
    own = pl.ds(pl.multiple_of(me * tiles, tiles), tiles)
    load_calendar = pltpu.make_async_copy(calendar, calendars.at[own], in_sems.at[1])
    load_lags = pltpu.make_async_copy(lags, lags_ref, in_sems.at[2])
    load_calendar.start()
    load_events.start()
    load_lags.start()
    lax.fori_loop(0, chunks, lambda c, _: (load(c).start(), 0)[1], 0)

    def send_calendar(i):
        return pltpu.make_async_remote_copy(
            calendars.at[own], calendars.at[own], n_send.at[i - 1], n_recv.at[i - 1],
            device_id={"tm": lax.rem(me + i, tm)},
        )

    def send_sums(i):
        return pltpu.make_async_remote_copy(
            sums, got_sums.at[i - 1], m_send.at[i - 1], m_recv.at[i - 1],
            device_id={"space": lax.rem(here + i, space)},
        )

    def send_totals(i):
        return pltpu.make_async_remote_copy(
            totals, got_totals.at[i - 1], t_send.at[i - 1], t_recv.at[i - 1],
            device_id={"tm": lax.rem(me + i, tm)},
        )

    def bits_of(turn):
        return [1 << ((turn * stages // TURNS + stage) % stages) for stage in range(stages)]

    half_rows = rows // TURNS

    def leaving(turn, stage):
        bits = bits_of(turn)
        return [
            apart for apart in range(1, tm)
            if apart & bits[stage] and not any(apart & bit for bit in bits[:stage])
        ]

    def first_slot(stage):
        return tm - (tm >> stage)

    def send_codes(c, turn, stage):
        peer = {"tm": flip(me, bits_of(turn)[stage])}
        slots = pl.ds(first_slot(stage), tm >> (stage + 1))
        return (
            pltpu.make_async_remote_copy(
                codes.at[c, turn, slots], got_codes.at[c, turn, slots],
                c_send.at[stage, turn, c], c_recv.at[stage, turn, c], device_id=peer,
            ),
            pltpu.make_async_remote_copy(
                scales.at[c, turn, slots], got_scales.at[c, turn, slots],
                s_send.at[stage, turn, c], s_recv.at[stage, turn, c], device_id=peer,
            ),
        )

    load_calendar.wait()
    pl.semaphore_wait(barrier, tm - 1 + here)
    for i in range(1, tm):
        send_calendar(i).start()
    lax.fori_loop(0, here, answer, 0)
    load_events.wait()
    count_weights(2 * (events_ref[...] - me * days) + PAD, weights_ref, lag_count)
    count_days(events_ref[...] + PAD, counts_ref, lag_count)
    own_regressors(calendars[own, :], weights_ref)

    def multiply(c):
        load(c).wait()
        raws[c] = jnp.dot(weights_ref[...], xs[c].reshape(depth, CHUNK), preferred_element_type=jnp.float32)

    def each(body, start, stop):
        lax.fori_loop(start, stop, lambda c, _: (body(c), 0)[1], 0)

    each(multiply, 0, AHEAD)

    for i in range(1, tm):
        send_calendar(i).wait()
    design = jnp.concatenate(regressors(calendars[...]), axis=1).astype(jnp.bfloat16)
    system = jnp.concatenate(
        [
            lax.dot_general(design, side, NT, preferred_element_type=jnp.float32)
            for side in (counts_ref[...], design)
        ],
        axis=1,
    )
    fit = solve(system, maps)
    high, middle, low = [piece.astype(jnp.float32) for piece in split3(fit)]
    left[...] = jnp.transpose(jnp.concatenate([high, high, high, middle, middle, low], axis=0)).astype(jnp.bfloat16)
    spatial[...] = jnp.zeros_like(spatial)

    def post(c, stage):
        for turn in range(TURNS):
            lines = slice(turn * half_rows, (turn + 1) * half_rows)
            for slot, apart in enumerate(leaving(turn, stage)):
                place = first_slot(stage) + slot
                codes[c, turn, place], scales[c, turn, place] = encode(parts[apart, c, lines])
            for copy in send_codes(c, turn, stage):
                copy.start()

    def collect(c, stage):
        for turn in range(TURNS):
            bit = bits_of(turn)[stage]
            lines = slice(turn * half_rows, (turn + 1) * half_rows)
            for copy in send_codes(c, turn, stage):
                copy.wait_recv()
            for slot, apart in enumerate(leaving(turn, stage)):
                place = first_slot(stage) + slot
                parts[apart - bit, c, lines] += decode(got_codes[c, turn, place], got_scales[c, turn, place])

    def anomalies(c):
        seasonal = []
        for variable in range(2):
            start = count_rows + 16 * variable
            p_high, p_middle, p_low = split3(raws[c, start : start + 16, :])
            right = jnp.concatenate([p_high, p_middle, p_low, p_high, p_middle, p_high], axis=0)
            product = jnp.dot(left[...], right, preferred_element_type=jnp.float32)
            seasonal.append(product.reshape(types, 1, lag_count, CHUNK))
        seasonal = jnp.concatenate(seasonal, axis=1).reshape(count_rows, CHUNK)
        whole[...] = raws[c, :count_rows, :] - seasonal
        for apart in range(tm):
            parts[apart, c] = whole[pl.ds(pl.multiple_of(flip(me, apart) * rows, rows), rows), :]
        post(c, 0)
        spatial[...] += whole[...]

    def both(c):
        anomalies(c)
        multiply(c + AHEAD)

    each(both, 0, chunks - AHEAD)
    each(anomalies, chunks - AHEAD, chunks)

    ones = jnp.ones((8, CHUNK), jnp.bfloat16)
    total = jnp.zeros((8, count_rows), jnp.float32)
    for piece in split3(spatial[...]):
        total = total + lax.dot_general(ones, piece, NT, preferred_element_type=jnp.float32)
    sums[...] = total[0:1, :]

    @pl.when(here < space - 1)
    def _():
        pl.semaphore_wait(ready, space - 1 - here)

    for i in range(1, space):
        send_sums(i).start()

    load_lags.wait()
    target = lax.broadcasted_iota(jnp.int32, (rows, rows), 0)
    source = lax.broadcasted_iota(jnp.int32, (rows, rows), 1)
    group = 2 * lag_count
    assert group & (group - 1) == 0
    inside = lax.bitwise_and(target, group - 1)
    base = target - inside + lax.bitwise_and(target, 1) * lag_count
    place = lax.shift_right_logical(inside, 1)
    wanted = base
    for lag in range(lag_count):
        wanted = jnp.where(place == lag, base + lags_ref[lag], wanted)
    order[...] = ones_where(source == wanted)

    half = chunks // 4

    def relay(stage):
        def body(c):
            collect(c, stage - 1)
            post(c, stage)

        return body

    def spread_sums():
        total = sums[...]
        for i in range(1, space):
            send_sums(i).wait()
            total = total + got_sums[i - 1]
        totals[...] = total
        for i in range(1, tm):
            send_totals(i).start()

    for stage in range(1, stages):
        each(relay(stage), 0, half)
        if stage == 1:
            spread_sums()
        each(relay(stage), half, chunks)

    total = totals[...]
    for i in range(1, tm):
        send_totals(i).wait()
        total = total + got_totals[i - 1]
    means[...] = lax.dot_general(
        jnp.broadcast_to(total * (1.0 / (8 * members * all_points)), (8, count_rows)), jnp.ones((8, CHUNK), jnp.float32),
        TN, precision=lax.Precision.HIGHEST, preferred_element_type=jnp.float32,
    )


    def gather(c):
        collect(c, stages - 1)
        mean = means[pl.ds(pl.multiple_of(me * rows, rows), rows), :]
        value = parts[0, c] * (1.0 / members) - mean
        placed = sum(jnp.dot(order[...], piece, preferred_element_type=jnp.float32) for piece in split3(value))
        columns = pl.ds(pl.multiple_of(c * CHUNK, CHUNK), CHUNK)
        out_ref[:, :, :, columns] = placed.reshape(out_ref.shape[:3] + (CHUNK,))

    each(gather, 0, chunks)

    def sent(c):
        for turn in range(TURNS):
            for stage in range(stages):
                for copy in send_codes(c, turn, stage):
                    copy.wait_send()

    each(sent, 0, chunks)


def shards(tm, space, fields, calendar_day, events, lag_offsets):
    types, members = events.shape
    lag_count = lag_offsets.shape[0]
    days, variables, points = fields.shape
    depth = variables * days
    count_rows = types * lag_count * variables
    rows = count_rows // tm
    chunks = points // CHUNK
    sent = (chunks, TURNS, tm - 1)
    copies = (tm.bit_length() - 1, TURNS, chunks)
    dma = pltpu.SemaphoreType.DMA
    vmem = pltpu.VMEM
    f32, bf16 = jnp.float32, jnp.bfloat16
    shape = (types // tm, lag_count, variables, points)
    in_hbm = [
        pltpu.with_memory_space_constraint(value, pltpu.HBM)
        for value in (calendar_day.reshape(days // LANES, LANES), events, lag_offsets)
    ]
    return pl.pallas_call(
        functools.partial(compose, tm, space, members, points * space),
        out_shape=jax.ShapeDtypeStruct(shape, f32),
        in_specs=[pl.BlockSpec(memory_space=pltpu.HBM)] * 4,
        out_specs=pl.BlockSpec(memory_space=vmem),
        scratch_shapes=[
            vmem((chunks, days, variables, CHUNK), bf16),
            vmem((tm * days // LANES, LANES), jnp.int32),
            vmem((types, members), jnp.int32),
            pltpu.SMEM((lag_count,), jnp.int32),
            vmem((count_rows + 32, depth), bf16),
            vmem((types * lag_count, tm * days), bf16),
            vmem((types * lag_count, 96), bf16),
            vmem((chunks, count_rows + 32, CHUNK), f32),
            vmem((count_rows, CHUNK), f32),
            vmem((count_rows, CHUNK), f32),
            vmem((tm, chunks, rows, CHUNK), f32),
            vmem((rows, rows), bf16),
            vmem((1, count_rows), f32),
            vmem((space - 1, 1, count_rows), f32),
            vmem((1, count_rows), f32),
            vmem((tm - 1, 1, count_rows), f32),
            vmem((count_rows, CHUNK), f32),
            vmem(sent + (rows // TURNS, CHUNK), jnp.int16),
            vmem(sent + (1, CHUNK), f32),
            vmem(sent + (rows // TURNS, CHUNK), jnp.int16),
            vmem(sent + (1, CHUNK), f32),
            pltpu.SemaphoreType.REGULAR,
            dma((chunks,)), dma((3,)),
            dma((tm - 1,)), dma((tm - 1,)),
            dma((space - 1,)), dma((space - 1,)),
            dma((tm - 1,)), dma((tm - 1,)),
            dma(copies), dma(copies), dma(copies), dma(copies),
        ],
        compiler_params=pltpu.CompilerParams(
            collective_id=0, has_side_effects=True, vmem_limit_bytes=52 * 2**20
        ),
        name="compose",
    )(fields, *in_hbm)


def solution(mesh):
    return jax.shard_map(
        functools.partial(shards, mesh.shape["tm"], mesh.shape["space"]),
        mesh=mesh,
        in_specs=(P("tm", None, "space"), P("tm"), P(), P()),
        out_specs=P("tm", None, None, "space"),
        check_vma=False,
    )
```

```python
import functools

import jax
import jax.numpy as jnp
from jax import lax
from jax.experimental import pallas as pl
from jax.experimental.pallas import tpu as pltpu
from jax.sharding import PartitionSpec as P

HARMONICS = 4
TERMS = 2 * HARMONICS + 1
TWO_PI = 6.283185307179586
LANES = 128
PAD = 128
CHUNK = 512
AHEAD = 1
TURNS = 2
NN = (((1,), (0,)), ((), ()))
NT = (((1,), (1,)), ((), ()))
TN = (((0,), (0,)), ((), ()))


def split3(value):
    high = value.astype(jnp.bfloat16)
    rest = value - high.astype(jnp.float32)
    middle = rest.astype(jnp.bfloat16)
    low = (rest - middle.astype(jnp.float32)).astype(jnp.bfloat16)
    return high, middle, low


def encode(part):
    top = jnp.max(jnp.abs(part), axis=0, keepdims=True)
    factor = jnp.where(top > 0.0, 32767.0 / jnp.where(top > 0.0, top, 1.0), 0.0)
    return jnp.round(part * factor).astype(jnp.int32).astype(jnp.int16), top * (1.0 / 32767.0)


def decode(codes, scale):
    return codes.astype(jnp.int32).astype(jnp.float32) * scale


def flip(index, bits):
    bit = 1
    flipped = index
    while bit <= bits:
        if bits & bit:
            flipped = flipped + bit - 2 * bit * lax.rem(lax.div(index, bit), 2)
        bit *= 2
    return flipped


def ones_where(condition):
    return jnp.where(condition, 1.0, 0.0).astype(jnp.bfloat16)


def histograms(places, tiles):
    members = places.shape[1]
    upper = lax.shift_right_arithmetic(places, 7)
    lower = lax.bitwise_and(places, LANES - 1)
    tile_lines = lax.broadcasted_iota(jnp.int32, (-(-tiles // 8) * 8, members), 0)
    lane_lines = lax.broadcasted_iota(jnp.int32, (LANES, members), 0)
    for kind in range(places.shape[0]):
        in_tile = ones_where(upper[kind : kind + 1, :] == tile_lines)
        in_lane = ones_where(lower[kind : kind + 1, :] == lane_lines)
        yield lax.dot_general(in_tile, in_lane, NT, preferred_element_type=jnp.float32)


def widen(histogram, tiles, lines):
    return jnp.concatenate(
        [jnp.broadcast_to(histogram[tile : tile + 1, :], (lines, LANES)) for tile in range(tiles)], axis=1
    )


def count_weights(places, weights_ref, lag_count):
    tiles = (weights_ref.shape[1] + PAD) // LANES
    for kind, histogram in enumerate(histograms(places, tiles)):
        wide = widen(histogram, tiles, lag_count)
        for variable in range(2):
            rolled = pltpu.roll(wide, variable, 1, stride=2, stride_axis=0)
            start = (2 * kind + variable) * lag_count
            weights_ref[start : start + lag_count, :] = rolled[:, PAD:].astype(jnp.bfloat16)


def count_days(places, counts_ref, lag_count):
    tiles = (counts_ref.shape[1] + PAD) // LANES
    for kind, histogram in enumerate(histograms(places, tiles)):
        rolled = pltpu.roll(widen(histogram, tiles, lag_count), 0, 1, stride=1, stride_axis=0)
        counts_ref[kind * lag_count : (kind + 1) * lag_count, :] = rolled[:, PAD:].astype(jnp.bfloat16)


def regressors(calendar):
    phase = calendar.astype(jnp.float32) * (TWO_PI / 365.25)
    cosines, sines = [jnp.cos(phase)], [jnp.sin(phase)]
    for order in range(2, HARMONICS + 1):
        a, b = order // 2 - 1, order - order // 2 - 1
        cosines.append(cosines[a] * cosines[b] - sines[a] * sines[b])
        sines.append(sines[a] * cosines[b] + cosines[a] * sines[b])
    terms = [jnp.ones_like(phase)]
    for order in range(HARMONICS):
        terms += [cosines[order], sines[order]]
    line = lax.broadcasted_iota(jnp.int32, (16, LANES), 0)
    blocks = []
    for tile in range(calendar.shape[0]):
        block = jnp.zeros((16, LANES), jnp.float32)
        for term, values in enumerate(terms):
            block = jnp.where(line == term, values[tile : tile + 1, :], block)
        blocks.append(block)
    return blocks


def own_regressors(calendar, weights_ref):
    tiles = calendar.shape[0]
    stacked = jnp.concatenate(regressors(calendar), axis=0).astype(jnp.bfloat16)
    day = lax.broadcasted_iota(jnp.int32, (LANES, 2 * LANES), 0)
    place = lax.broadcasted_iota(jnp.int32, (LANES, 2 * LANES), 1)
    start = weights_ref.shape[0] - 32
    for variable in range(2):
        spread = jnp.dot(stacked, ones_where(place == 2 * day + variable), preferred_element_type=jnp.float32)
        lines = jnp.concatenate([spread[16 * tile : 16 * tile + 16, :] for tile in range(tiles)], axis=1)
        weights_ref[start + 16 * variable : start + 16 * variable + 16, :] = lines.astype(jnp.bfloat16)


def solve(system, sides_width):
    lines = lax.broadcasted_iota(jnp.int32, (16, LANES), 0)
    columns = [
        jnp.broadcast_to(system[:, sides_width + k : sides_width + k + 1], (16, LANES)) for k in range(TERMS)
    ]
    sides = [system[:, start : start + LANES] for start in range(0, sides_width, LANES)]
    for k in range(TERMS):
        column = columns[k]
        inverse = 1.0 / column[k : k + 1, :]

        def eliminate(block):
            pivot = block[k : k + 1, :] * inverse
            return jnp.where(lines == k, pivot, block - column * pivot)

        sides = [eliminate(block) for block in sides]
        columns = [eliminate(block) if j > k else block for j, block in enumerate(columns)]
    return jnp.concatenate([jnp.where(lines < TERMS, block, 0.0) for block in sides], axis=1)


def compose(
    tm, space, members, all_points,
    fields, calendar, events, lags, out_ref,
    xs, calendars, events_ref, lags_ref, weights_ref, counts_ref, left, raws, whole, spatial, parts, order,
    sums, got_sums, totals, got_totals, means, codes, scales, got_codes, got_scales,
    ready, x_sems, in_sems, n_send, n_recv, m_send, m_recv, t_send, t_recv, c_send, c_recv, s_send, s_recv,
):
    chunks, days = xs.shape[0], xs.shape[1]
    depth = weights_ref.shape[1]
    count_rows = weights_ref.shape[0] - 32
    rows = count_rows // tm
    types = events_ref.shape[0]
    lag_count = lags_ref.shape[0]
    maps = types * lag_count
    me = lax.axis_index("tm")
    here = lax.axis_index("space")
    stages = tm.bit_length() - 1

    def load(c):
        return pltpu.make_async_copy(
            fields.at[:, :, pl.ds(pl.multiple_of(c * CHUNK, CHUNK), CHUNK)], xs.at[c], x_sems.at[c]
        )

    barrier = pltpu.get_barrier_semaphore()
    for i in range(1, tm):
        pl.semaphore_signal(barrier, inc=1, device_id={"tm": lax.rem(me + i, tm)})

    def greet(place, carry):
        pl.semaphore_signal(barrier, inc=1, device_id={"space": place})
        return carry

    def answer(place, carry):
        pl.semaphore_signal(ready, inc=1, device_id={"space": place})
        return carry

    lax.fori_loop(here + 1, space, greet, 0)
    load_events = pltpu.make_async_copy(events, events_ref, in_sems.at[0])
    tiles = days // LANES
    own = pl.ds(pl.multiple_of(me * tiles, tiles), tiles)
    load_calendar = pltpu.make_async_copy(calendar, calendars.at[own], in_sems.at[1])
    load_lags = pltpu.make_async_copy(lags, lags_ref, in_sems.at[2])
    load_calendar.start()
    load_events.start()
    load_lags.start()
    lax.fori_loop(0, chunks, lambda c, _: (load(c).start(), 0)[1], 0)

    def send_calendar(i):
        return pltpu.make_async_remote_copy(
            calendars.at[own], calendars.at[own], n_send.at[i - 1], n_recv.at[i - 1],
            device_id={"tm": lax.rem(me + i, tm)},
        )

    def send_sums(i):
        return pltpu.make_async_remote_copy(
            sums, got_sums.at[i - 1], m_send.at[i - 1], m_recv.at[i - 1],
            device_id={"space": lax.rem(here + i, space)},
        )

    def send_totals(i):
        return pltpu.make_async_remote_copy(
            totals, got_totals.at[i - 1], t_send.at[i - 1], t_recv.at[i - 1],
            device_id={"tm": lax.rem(me + i, tm)},
        )

    def bits_of(turn):
        return [1 << ((turn * stages // TURNS + stage) % stages) for stage in range(stages)]

    half_rows = rows // TURNS

    def leaving(turn, stage):
        bits = bits_of(turn)
        return [
            apart for apart in range(1, tm)
            if apart & bits[stage] and not any(apart & bit for bit in bits[:stage])
        ]

    def first_slot(stage):
        return tm - (tm >> stage)

    def send_codes(c, turn, stage):
        peer = {"tm": flip(me, bits_of(turn)[stage])}
        slots = pl.ds(first_slot(stage), tm >> (stage + 1))
        return (
            pltpu.make_async_remote_copy(
                codes.at[c, turn, slots], got_codes.at[c, turn, slots],
                c_send.at[stage, turn, c], c_recv.at[stage, turn, c], device_id=peer,
            ),
            pltpu.make_async_remote_copy(
                scales.at[c, turn, slots], got_scales.at[c, turn, slots],
                s_send.at[stage, turn, c], s_recv.at[stage, turn, c], device_id=peer,
            ),
        )

    load_calendar.wait()
    pl.semaphore_wait(barrier, tm - 1 + here)
    for i in range(1, tm):
        send_calendar(i).start()
    lax.fori_loop(0, here, answer, 0)
    load_events.wait()
    count_weights(2 * (events_ref[...] - me * days) + PAD, weights_ref, lag_count)
    count_days(events_ref[...] + PAD, counts_ref, lag_count)
    own_regressors(calendars[own, :], weights_ref)

    def multiply(c):
        load(c).wait()
        raws[c] = jnp.dot(weights_ref[...], xs[c].reshape(depth, CHUNK), preferred_element_type=jnp.float32)

    def each(body, start, stop):
        lax.fori_loop(start, stop, lambda c, _: (body(c), 0)[1], 0)

    each(multiply, 0, AHEAD)

    for i in range(1, tm):
        send_calendar(i).wait()
    design = jnp.concatenate(regressors(calendars[...]), axis=1).astype(jnp.bfloat16)
    system = jnp.concatenate(
        [
            lax.dot_general(design, side, NT, preferred_element_type=jnp.float32)
            for side in (counts_ref[...], design)
        ],
        axis=1,
    )
    fit = solve(system, maps)
    high, middle, low = [piece.astype(jnp.float32) for piece in split3(fit)]
    left[...] = jnp.transpose(jnp.concatenate([high, high, high, middle, middle, low], axis=0)).astype(jnp.bfloat16)
    spatial[...] = jnp.zeros_like(spatial)

    def post(c, stage, turns=range(TURNS)):
        for turn in turns:
            lines = slice(turn * half_rows, (turn + 1) * half_rows)
            for slot, apart in enumerate(leaving(turn, stage)):
                place = first_slot(stage) + slot
                codes[c, turn, place], scales[c, turn, place] = encode(parts[apart, c, lines])
            for copy in send_codes(c, turn, stage):
                copy.start()

    def collect(c, stage, turns=range(TURNS)):
        for turn in turns:
            bit = bits_of(turn)[stage]
            lines = slice(turn * half_rows, (turn + 1) * half_rows)
            for copy in send_codes(c, turn, stage):
                copy.wait_recv()
            for slot, apart in enumerate(leaving(turn, stage)):
                place = first_slot(stage) + slot
                parts[apart - bit, c, lines] += decode(got_codes[c, turn, place], got_scales[c, turn, place])

    def anomalies(c):
        seasonal = []
        for variable in range(2):
            start = count_rows + 16 * variable
            p_high, p_middle, p_low = split3(raws[c, start : start + 16, :])
            right = jnp.concatenate([p_high, p_middle, p_low, p_high, p_middle, p_high], axis=0)
            product = jnp.dot(left[...], right, preferred_element_type=jnp.float32)
            seasonal.append(product.reshape(types, 1, lag_count, CHUNK))
        seasonal = jnp.concatenate(seasonal, axis=1).reshape(count_rows, CHUNK)
        whole[...] = raws[c, :count_rows, :] - seasonal
        for apart in range(tm):
            parts[apart, c] = whole[pl.ds(pl.multiple_of(flip(me, apart) * rows, rows), rows), :]
        post(c, 0)
        spatial[...] += whole[...]

    def both(c):
        anomalies(c)
        multiply(c + AHEAD)

    each(both, 0, chunks - AHEAD)
    each(anomalies, chunks - AHEAD, chunks)

    ones = jnp.ones((8, CHUNK), jnp.bfloat16)
    total = jnp.zeros((8, count_rows), jnp.float32)
    for piece in split3(spatial[...]):
        total = total + lax.dot_general(ones, piece, NT, preferred_element_type=jnp.float32)
    sums[...] = total[0:1, :]

    @pl.when(here < space - 1)
    def _():
        pl.semaphore_wait(ready, space - 1 - here)

    for i in range(1, space):
        send_sums(i).start()

    load_lags.wait()
    target = lax.broadcasted_iota(jnp.int32, (rows, rows), 0)
    source = lax.broadcasted_iota(jnp.int32, (rows, rows), 1)
    group = 2 * lag_count
    assert group & (group - 1) == 0
    inside = lax.bitwise_and(target, group - 1)
    base = target - inside + lax.bitwise_and(target, 1) * lag_count
    place = lax.shift_right_logical(inside, 1)
    wanted = base
    for lag in range(lag_count):
        wanted = jnp.where(place == lag, base + lags_ref[lag], wanted)
    order[...] = ones_where(source == wanted)

    half = chunks // 4

    def relay(stage):
        def body(c):
            for turn in range(TURNS):
                collect(c, stage - 1, [turn])
                post(c, stage, [turn])

        return body

    def spread_sums():
        total = sums[...]
        for i in range(1, space):
            send_sums(i).wait()
            total = total + got_sums[i - 1]
        totals[...] = total
        for i in range(1, tm):
            send_totals(i).start()

    for stage in range(1, stages):
        each(relay(stage), 0, half)
        if stage == 1:
            spread_sums()
        each(relay(stage), half, chunks)

    total = totals[...]
    for i in range(1, tm):
        send_totals(i).wait()
        total = total + got_totals[i - 1]
    means[...] = lax.dot_general(
        jnp.broadcast_to(total * (1.0 / (8 * members * all_points)), (8, count_rows)), jnp.ones((8, LANES), jnp.float32),
        TN, precision=lax.Precision.HIGHEST, preferred_element_type=jnp.float32,
    )


    def gather(c):
        collect(c, stages - 1)
        mean = means[pl.ds(pl.multiple_of(me * rows, rows), rows), :]
        mean = jnp.concatenate([mean] * (CHUNK // LANES), axis=1)
        value = parts[0, c] * (1.0 / members) - mean
        placed = sum(jnp.dot(order[...], piece, preferred_element_type=jnp.float32) for piece in split3(value))
        columns = pl.ds(pl.multiple_of(c * CHUNK, CHUNK), CHUNK)
        out_ref[:, :, :, columns] = placed.reshape(out_ref.shape[:3] + (CHUNK,))

    each(gather, 0, chunks)

    def sent(c):
        for turn in range(TURNS):
            for stage in range(stages):
                for copy in send_codes(c, turn, stage):
                    copy.wait_send()

    each(sent, 0, chunks)


def shards(tm, space, fields, calendar_day, events, lag_offsets):
    types, members = events.shape
    lag_count = lag_offsets.shape[0]
    days, variables, points = fields.shape
    depth = variables * days
    count_rows = types * lag_count * variables
    rows = count_rows // tm
    chunks = points // CHUNK
    sent = (chunks, TURNS, tm - 1)
    copies = (tm.bit_length() - 1, TURNS, chunks)
    dma = pltpu.SemaphoreType.DMA
    vmem = pltpu.VMEM
    f32, bf16 = jnp.float32, jnp.bfloat16
    shape = (types // tm, lag_count, variables, points)
    in_hbm = [
        pltpu.with_memory_space_constraint(value, pltpu.HBM)
        for value in (calendar_day.reshape(days // LANES, LANES), events, lag_offsets)
    ]
    return pl.pallas_call(
        functools.partial(compose, tm, space, members, points * space),
        out_shape=jax.ShapeDtypeStruct(shape, f32),
        in_specs=[pl.BlockSpec(memory_space=pltpu.HBM)] * 4,
        out_specs=pl.BlockSpec(memory_space=vmem),
        scratch_shapes=[
            vmem((chunks, days, variables, CHUNK), bf16),
            vmem((tm * days // LANES, LANES), jnp.int32),
            vmem((types, members), jnp.int32),
            pltpu.SMEM((lag_count,), jnp.int32),
            vmem((count_rows + 32, depth), bf16),
            vmem((types * lag_count, tm * days), bf16),
            vmem((types * lag_count, 96), bf16),
            vmem((chunks, count_rows + 32, CHUNK), f32),
            vmem((count_rows, CHUNK), f32),
            vmem((count_rows, CHUNK), f32),
            vmem((tm, chunks, rows, CHUNK), f32),
            vmem((rows, rows), bf16),
            vmem((1, count_rows), f32),
            vmem((space - 1, 1, count_rows), f32),
            vmem((1, count_rows), f32),
            vmem((tm - 1, 1, count_rows), f32),
            vmem((count_rows, LANES), f32),
            vmem(sent + (rows // TURNS, CHUNK), jnp.int16),
            vmem(sent + (1, CHUNK), f32),
            vmem(sent + (rows // TURNS, CHUNK), jnp.int16),
            vmem(sent + (1, CHUNK), f32),
            pltpu.SemaphoreType.REGULAR,
            dma((chunks,)), dma((3,)),
            dma((tm - 1,)), dma((tm - 1,)),
            dma((space - 1,)), dma((space - 1,)),
            dma((tm - 1,)), dma((tm - 1,)),
            dma(copies), dma(copies), dma(copies), dma(copies),
        ],
        compiler_params=pltpu.CompilerParams(
            collective_id=0, has_side_effects=True, vmem_limit_bytes=52 * 2**20
        ),
        name="compose",
    )(fields, *in_hbm)


def solution(mesh):
    return jax.shard_map(
        functools.partial(shards, mesh.shape["tm"], mesh.shape["space"]),
        mesh=mesh,
        in_specs=(P("tm", None, "space"), P("tm"), P(), P()),
        out_specs=P("tm", None, None, "space"),
        check_vma=False,
    )
```

```python
import functools

import jax
import jax.numpy as jnp
from jax import lax
from jax.experimental import pallas as pl
from jax.experimental.pallas import tpu as pltpu
from jax.sharding import PartitionSpec as P

HARMONICS = 4
TERMS = 2 * HARMONICS + 1
TWO_PI = 6.283185307179586
LANES = 128
PAD = 128
CHUNK = 512
AHEAD = 1
TURNS = 2
NN = (((1,), (0,)), ((), ()))
NT = (((1,), (1,)), ((), ()))
TN = (((0,), (0,)), ((), ()))


def split3(value):
    high = value.astype(jnp.bfloat16)
    rest = value - high.astype(jnp.float32)
    middle = rest.astype(jnp.bfloat16)
    low = (rest - middle.astype(jnp.float32)).astype(jnp.bfloat16)
    return high, middle, low


def encode(part):
    top = jnp.max(jnp.abs(part), axis=0, keepdims=True)
    factor = jnp.where(top > 0.0, 32767.0 / jnp.where(top > 0.0, top, 1.0), 0.0)
    return jnp.round(part * factor).astype(jnp.int32).astype(jnp.int16), top * (1.0 / 32767.0)


def decode(codes, scale):
    return codes.astype(jnp.int32).astype(jnp.float32) * scale


def flip(index, bits):
    bit = 1
    flipped = index
    while bit <= bits:
        if bits & bit:
            flipped = flipped + bit - 2 * bit * lax.rem(lax.div(index, bit), 2)
        bit *= 2
    return flipped


def ones_where(condition):
    return jnp.where(condition, 1.0, 0.0).astype(jnp.bfloat16)


def histograms(places, tiles):
    members = places.shape[1]
    upper = lax.shift_right_arithmetic(places, 7)
    lower = lax.bitwise_and(places, LANES - 1)
    tile_lines = lax.broadcasted_iota(jnp.int32, (-(-tiles // 8) * 8, members), 0)
    lane_lines = lax.broadcasted_iota(jnp.int32, (LANES, members), 0)
    for kind in range(places.shape[0]):
        in_tile = ones_where(upper[kind : kind + 1, :] == tile_lines)
        in_lane = ones_where(lower[kind : kind + 1, :] == lane_lines)
        yield lax.dot_general(in_tile, in_lane, NT, preferred_element_type=jnp.float32)


def widen(histogram, tiles, lines):
    return jnp.concatenate(
        [jnp.broadcast_to(histogram[tile : tile + 1, :], (lines, LANES)) for tile in range(tiles)], axis=1
    )


def count_weights(places, weights_ref, lag_count):
    tiles = (weights_ref.shape[1] + PAD) // LANES
    for kind, histogram in enumerate(histograms(places, tiles)):
        wide = widen(histogram, tiles, lag_count)
        for variable in range(2):
            rolled = pltpu.roll(wide, variable, 1, stride=2, stride_axis=0)
            start = (2 * kind + variable) * lag_count
            weights_ref[start : start + lag_count, :] = rolled[:, PAD:].astype(jnp.bfloat16)


def count_days(places, counts_ref, lag_count):
    tiles = (counts_ref.shape[1] + PAD) // LANES
    for kind, histogram in enumerate(histograms(places, tiles)):
        rolled = pltpu.roll(widen(histogram, tiles, lag_count), 0, 1, stride=1, stride_axis=0)
        counts_ref[kind * lag_count : (kind + 1) * lag_count, :] = rolled[:, PAD:].astype(jnp.bfloat16)


def regressors(calendar):
    phase = calendar.astype(jnp.float32) * (TWO_PI / 365.25)
    cosines, sines = [jnp.cos(phase)], [jnp.sin(phase)]
    for order in range(2, HARMONICS + 1):
        a, b = order // 2 - 1, order - order // 2 - 1
        cosines.append(cosines[a] * cosines[b] - sines[a] * sines[b])
        sines.append(sines[a] * cosines[b] + cosines[a] * sines[b])
    terms = [jnp.ones_like(phase)]
    for order in range(HARMONICS):
        terms += [cosines[order], sines[order]]
    line = lax.broadcasted_iota(jnp.int32, (16, LANES), 0)
    blocks = []
    for tile in range(calendar.shape[0]):
        block = jnp.zeros((16, LANES), jnp.float32)
        for term, values in enumerate(terms):
            block = jnp.where(line == term, values[tile : tile + 1, :], block)
        blocks.append(block)
    return blocks


def own_regressors(calendar, weights_ref):
    tiles = calendar.shape[0]
    stacked = jnp.concatenate(regressors(calendar), axis=0).astype(jnp.bfloat16)
    day = lax.broadcasted_iota(jnp.int32, (LANES, 2 * LANES), 0)
    place = lax.broadcasted_iota(jnp.int32, (LANES, 2 * LANES), 1)
    start = weights_ref.shape[0] - 32
    for variable in range(2):
        spread = jnp.dot(stacked, ones_where(place == 2 * day + variable), preferred_element_type=jnp.float32)
        lines = jnp.concatenate([spread[16 * tile : 16 * tile + 16, :] for tile in range(tiles)], axis=1)
        weights_ref[start + 16 * variable : start + 16 * variable + 16, :] = lines.astype(jnp.bfloat16)


def solve(system, sides_width):
    lines = lax.broadcasted_iota(jnp.int32, (16, LANES), 0)
    columns = [
        jnp.broadcast_to(system[:, sides_width + k : sides_width + k + 1], (16, LANES)) for k in range(TERMS)
    ]
    sides = [system[:, start : start + LANES] for start in range(0, sides_width, LANES)]
    for k in range(TERMS):
        column = columns[k]
        inverse = 1.0 / column[k : k + 1, :]

        def eliminate(block):
            pivot = block[k : k + 1, :] * inverse
            return jnp.where(lines == k, pivot, block - column * pivot)

        sides = [eliminate(block) for block in sides]
        columns = [eliminate(block) if j > k else block for j, block in enumerate(columns)]
    return jnp.concatenate([jnp.where(lines < TERMS, block, 0.0) for block in sides], axis=1)


def compose(
    tm, space, members, all_points,
    fields, calendar, events, lags, out_ref,
    xs, calendars, events_ref, lags_ref, weights_ref, counts_ref, left, raws, whole, spatial, parts, order,
    sums, got_sums, totals, got_totals, means, codes, scales, got_codes, got_scales,
    ready, x_sems, in_sems, n_send, n_recv, m_send, m_recv, t_send, t_recv, c_send, c_recv, s_send, s_recv,
):
    chunks, days = xs.shape[0], xs.shape[1]
    depth = weights_ref.shape[1]
    count_rows = weights_ref.shape[0] - 32
    rows = count_rows // tm
    types = events_ref.shape[0]
    lag_count = lags_ref.shape[0]
    maps = types * lag_count
    me = lax.axis_index("tm")
    here = lax.axis_index("space")
    stages = tm.bit_length() - 1

    def load(c):
        return pltpu.make_async_copy(
            fields.at[:, :, pl.ds(pl.multiple_of(c * CHUNK, CHUNK), CHUNK)], xs.at[c], x_sems.at[c]
        )

    barrier = pltpu.get_barrier_semaphore()
    for i in range(1, tm):
        pl.semaphore_signal(barrier, inc=1, device_id={"tm": lax.rem(me + i, tm)})

    def greet(place, carry):
        pl.semaphore_signal(barrier, inc=1, device_id={"space": place})
        return carry

    def answer(place, carry):
        pl.semaphore_signal(ready, inc=1, device_id={"space": place})
        return carry

    lax.fori_loop(here + 1, space, greet, 0)
    load_events = pltpu.make_async_copy(events, events_ref, in_sems.at[0])
    tiles = days // LANES
    own = pl.ds(pl.multiple_of(me * tiles, tiles), tiles)
    load_calendar = pltpu.make_async_copy(calendar, calendars.at[own], in_sems.at[1])
    load_lags = pltpu.make_async_copy(lags, lags_ref, in_sems.at[2])
    load_calendar.start()
    load_events.start()
    load_lags.start()
    lax.fori_loop(0, chunks, lambda c, _: (load(c).start(), 0)[1], 0)

    def send_calendar(i):
        return pltpu.make_async_remote_copy(
            calendars.at[own], calendars.at[own], n_send.at[i - 1], n_recv.at[i - 1],
            device_id={"tm": lax.rem(me + i, tm)},
        )

    def send_sums(i):
        return pltpu.make_async_remote_copy(
            sums, got_sums.at[i - 1], m_send.at[i - 1], m_recv.at[i - 1],
            device_id={"space": lax.rem(here + i, space)},
        )

    def send_totals(i):
        return pltpu.make_async_remote_copy(
            totals, got_totals.at[i - 1], t_send.at[i - 1], t_recv.at[i - 1],
            device_id={"tm": lax.rem(me + i, tm)},
        )

    def bits_of(turn):
        return [1 << ((turn * stages // TURNS + stage) % stages) for stage in range(stages)]

    half_rows = rows // TURNS

    def leaving(turn, stage):
        bits = bits_of(turn)
        return [
            apart for apart in range(1, tm)
            if apart & bits[stage] and not any(apart & bit for bit in bits[:stage])
        ]

    def first_slot(stage):
        return tm - (tm >> stage)

    def send_codes(c, turn, stage):
        peer = {"tm": flip(me, bits_of(turn)[stage])}
        slots = pl.ds(first_slot(stage), tm >> (stage + 1))
        return (
            pltpu.make_async_remote_copy(
                codes.at[c, turn, slots], got_codes.at[c, turn, slots],
                c_send.at[stage, turn, c], c_recv.at[stage, turn, c], device_id=peer,
            ),
            pltpu.make_async_remote_copy(
                scales.at[c, turn, slots], got_scales.at[c, turn, slots],
                s_send.at[stage, turn, c], s_recv.at[stage, turn, c], device_id=peer,
            ),
        )

    load_calendar.wait()
    pl.semaphore_wait(barrier, tm - 1 + here)
    for i in range(1, tm):
        send_calendar(i).start()
    lax.fori_loop(0, here, answer, 0)
    load_events.wait()
    count_weights(2 * (events_ref[...] - me * days) + PAD, weights_ref, lag_count)
    count_days(events_ref[...] + PAD, counts_ref, lag_count)
    own_regressors(calendars[own, :], weights_ref)

    def multiply(c):
        load(c).wait()
        raws[c] = jnp.dot(weights_ref[...], xs[c].reshape(depth, CHUNK), preferred_element_type=jnp.float32)

    def each(body, start, stop):
        lax.fori_loop(start, stop, lambda c, _: (body(c), 0)[1], 0)

    each(multiply, 0, AHEAD)

    for i in range(1, tm):
        send_calendar(i).wait()
    design = jnp.concatenate(regressors(calendars[...]), axis=1).astype(jnp.bfloat16)
    system = jnp.concatenate(
        [
            lax.dot_general(design, side, NT, preferred_element_type=jnp.float32)
            for side in (counts_ref[...], design)
        ],
        axis=1,
    )
    fit = solve(system, maps)
    high, middle, low = [piece.astype(jnp.float32) for piece in split3(fit)]
    left[...] = jnp.transpose(jnp.concatenate([high, high, high, middle, middle, low], axis=0)).astype(jnp.bfloat16)
    spatial[...] = jnp.zeros_like(spatial)

    def post(c, stage):
        for turn in range(TURNS):
            lines = slice(turn * half_rows, (turn + 1) * half_rows)
            for slot, apart in enumerate(leaving(turn, stage)):
                place = first_slot(stage) + slot
                codes[c, turn, place], scales[c, turn, place] = encode(parts[apart, c, lines])
            for copy in send_codes(c, turn, stage):
                copy.start()

    def collect(c, stage):
        for turn in range(TURNS):
            bit = bits_of(turn)[stage]
            lines = slice(turn * half_rows, (turn + 1) * half_rows)
            for copy in send_codes(c, turn, stage):
                copy.wait_recv()
            for slot, apart in enumerate(leaving(turn, stage)):
                place = first_slot(stage) + slot
                parts[apart - bit, c, lines] += decode(got_codes[c, turn, place], got_scales[c, turn, place])

    def anomalies(c):
        seasonal = []
        for variable in range(2):
            start = count_rows + 16 * variable
            p_high, p_middle, p_low = split3(raws[c, start : start + 16, :])
            right = jnp.concatenate([p_high, p_middle, p_low, p_high, p_middle, p_high], axis=0)
            product = jnp.dot(left[...], right, preferred_element_type=jnp.float32)
            seasonal.append(product.reshape(types, 1, lag_count, CHUNK))
        seasonal = jnp.concatenate(seasonal, axis=1).reshape(count_rows, CHUNK)
        whole[...] = raws[c, :count_rows, :] - seasonal
        for apart in range(tm):
            parts[apart, c] = whole[pl.ds(pl.multiple_of(flip(me, apart) * rows, rows), rows), :]
        post(c, 0)
        spatial[...] += whole[...]

    def both(c):
        anomalies(c)
        multiply(c + AHEAD)

    each(both, 0, chunks - AHEAD)
    each(anomalies, chunks - AHEAD, chunks)

    ones = jnp.ones((8, CHUNK), jnp.bfloat16)
    total = jnp.zeros((8, count_rows), jnp.float32)
    for piece in split3(spatial[...]):
        total = total + lax.dot_general(ones, piece, NT, preferred_element_type=jnp.float32)
    sums[...] = total[0:1, :]

    @pl.when(here < space - 1)
    def _():
        pl.semaphore_wait(ready, space - 1 - here)

    for i in range(1, space):
        send_sums(i).start()

    load_lags.wait()
    target = lax.broadcasted_iota(jnp.int32, (rows, rows), 0)
    source = lax.broadcasted_iota(jnp.int32, (rows, rows), 1)
    group = 2 * lag_count
    assert group & (group - 1) == 0
    inside = lax.bitwise_and(target, group - 1)
    base = target - inside + lax.bitwise_and(target, 1) * lag_count
    place = lax.shift_right_logical(inside, 1)
    wanted = base
    for lag in range(lag_count):
        wanted = jnp.where(place == lag, base + lags_ref[lag], wanted)
    order[...] = ones_where(source == wanted)

    half = chunks // 4

    def relay(stage):
        def body(c):
            collect(c, stage - 1)
            post(c, stage)

        return body

    def spread_sums():
        total = sums[...]
        for i in range(1, space):
            send_sums(i).wait()
            total = total + got_sums[i - 1]
        totals[...] = total
        for i in range(1, tm):
            send_totals(i).start()

    for stage in range(1, stages):
        each(relay(stage), 0, half)
        if stage == 1:
            spread_sums()
        each(relay(stage), half, chunks)

    total = totals[...]
    for i in range(1, tm):
        send_totals(i).wait()
        total = total + got_totals[i - 1]
    means[...] = lax.dot_general(
        jnp.broadcast_to(total * (1.0 / (8 * members * all_points)), (8, count_rows)), jnp.ones((8, CHUNK), jnp.float32),
        TN, precision=lax.Precision.HIGHEST, preferred_element_type=jnp.float32,
    )


    def gather(c):
        pieces = []
        for turn in range(TURNS):
            for copy in send_codes(c, turn, stages - 1):
                copy.wait_recv()
            lines = slice(turn * half_rows, (turn + 1) * half_rows)
            place = first_slot(stages - 1)
            pieces.append(parts[0, c, lines] + decode(got_codes[c, turn, place], got_scales[c, turn, place]))
        mean = means[pl.ds(pl.multiple_of(me * rows, rows), rows), :]
        value = jnp.concatenate(pieces, axis=0) * (1.0 / members) - mean
        placed = sum(jnp.dot(order[...], piece, preferred_element_type=jnp.float32) for piece in split3(value))
        columns = pl.ds(pl.multiple_of(c * CHUNK, CHUNK), CHUNK)
        out_ref[:, :, :, columns] = placed.reshape(out_ref.shape[:3] + (CHUNK,))

    each(gather, 0, chunks)

    def sent(c):
        for turn in range(TURNS):
            for stage in range(stages):
                for copy in send_codes(c, turn, stage):
                    copy.wait_send()

    each(sent, 0, chunks)


def shards(tm, space, fields, calendar_day, events, lag_offsets):
    types, members = events.shape
    lag_count = lag_offsets.shape[0]
    days, variables, points = fields.shape
    depth = variables * days
    count_rows = types * lag_count * variables
    rows = count_rows // tm
    chunks = points // CHUNK
    sent = (chunks, TURNS, tm - 1)
    copies = (tm.bit_length() - 1, TURNS, chunks)
    dma = pltpu.SemaphoreType.DMA
    vmem = pltpu.VMEM
    f32, bf16 = jnp.float32, jnp.bfloat16
    shape = (types // tm, lag_count, variables, points)
    in_hbm = [
        pltpu.with_memory_space_constraint(value, pltpu.HBM)
        for value in (calendar_day.reshape(days // LANES, LANES), events, lag_offsets)
    ]
    return pl.pallas_call(
        functools.partial(compose, tm, space, members, points * space),
        out_shape=jax.ShapeDtypeStruct(shape, f32),
        in_specs=[pl.BlockSpec(memory_space=pltpu.HBM)] * 4,
        out_specs=pl.BlockSpec(memory_space=vmem),
        scratch_shapes=[
            vmem((chunks, days, variables, CHUNK), bf16),
            vmem((tm * days // LANES, LANES), jnp.int32),
            vmem((types, members), jnp.int32),
            pltpu.SMEM((lag_count,), jnp.int32),
            vmem((count_rows + 32, depth), bf16),
            vmem((types * lag_count, tm * days), bf16),
            vmem((types * lag_count, 96), bf16),
            vmem((chunks, count_rows + 32, CHUNK), f32),
            vmem((count_rows, CHUNK), f32),
            vmem((count_rows, CHUNK), f32),
            vmem((tm, chunks, rows, CHUNK), f32),
            vmem((rows, rows), bf16),
            vmem((1, count_rows), f32),
            vmem((space - 1, 1, count_rows), f32),
            vmem((1, count_rows), f32),
            vmem((tm - 1, 1, count_rows), f32),
            vmem((count_rows, CHUNK), f32),
            vmem(sent + (rows // TURNS, CHUNK), jnp.int16),
            vmem(sent + (1, CHUNK), f32),
            vmem(sent + (rows // TURNS, CHUNK), jnp.int16),
            vmem(sent + (1, CHUNK), f32),
            pltpu.SemaphoreType.REGULAR,
            dma((chunks,)), dma((3,)),
            dma((tm - 1,)), dma((tm - 1,)),
            dma((space - 1,)), dma((space - 1,)),
            dma((tm - 1,)), dma((tm - 1,)),
            dma(copies), dma(copies), dma(copies), dma(copies),
        ],
        compiler_params=pltpu.CompilerParams(
            collective_id=0, has_side_effects=True, vmem_limit_bytes=52 * 2**20
        ),
        name="compose",
    )(fields, *in_hbm)


def solution(mesh):
    return jax.shard_map(
        functools.partial(shards, mesh.shape["tm"], mesh.shape["space"]),
        mesh=mesh,
        in_specs=(P("tm", None, "space"), P("tm"), P(), P()),
        out_specs=P("tm", None, None, "space"),
        check_vma=False,
    )
```
